32 devices in a mesh: tp: 32 (over z, y, x, core).
Axes of the slice: x: 2, y: 2, z: 4, core: 2. Of those that a mesh axis runs over, the one named last changes fastest.
Arguments:
- tok_ids: int32 [2, 512], replicated
- next_ids: int32 [2, 512], replicated
- seq_lens: int32 [512], replicated
- embed: bfloat16 [49152, 2048], P('tp')
- ln_gain: bfloat16 [2048], replicated
- w_in: bfloat16 [2048, 18688], P(None, 'tp')
- w_out: bfloat16 [10240, 2048], P('tp')
- final_gain: bfloat16 [2048], replicated
- k_cache: bfloat16 [512, 2048, 128], P('tp')
- v_cache: bfloat16 [512, 2048, 128], P('tp')
Outputs:
- output 1: float32 [2, 512], replicated
- output 2: bfloat16 [512, 2048, 128], P('tp')
- output 3: bfloat16 [512, 2048, 128], P('tp')
All inputs are finite; a program needn't handle non-finite values.
Results may differ from the reference program's by a relative error of at most 0.001.
Values are sent between devices in bfloat16 or wider.
A program may use at most 1 GiB of HBM per device.

```python
import jax
import jax.numpy as jnp
from jax import lax

D = 2048
HEADS = 16
HEAD = 128
FF = 8192
VOCAB = 49152
GROUP = 32
BATCH_DEV = 16
CACHE_LEN = 2048
NUM_STEPS = 2

BATCH = BATCH_DEV * GROUP
QKV_WIDTH = (HEADS + 2) * HEAD
ATTN_WIDTH = HEADS * HEAD
QKV_DEV = QKV_WIDTH // GROUP
ATTN_DEV = ATTN_WIDTH // GROUP
FF_DEV = FF // GROUP
IN_DEV = QKV_DEV + 2 * FF_DEV
OUT_DEV = ATTN_DEV + FF_DEV
IN_WIDTH = IN_DEV * GROUP
OUT_WIDTH = OUT_DEV * GROUP
MAP_ROWS = min(BATCH, 64)
MAP_COUNT = BATCH // MAP_ROWS
NORM_EPS = 1e-6
ROPE_BASE = 10000.0


def setup_inputs(seed: int = 0) -> dict:
    key_list = jax.random.split(jax.random.key(seed), 11)
    tok_ids = jax.random.randint(key_list[0], (NUM_STEPS, BATCH), 0, VOCAB, dtype=jnp.int32)
    next_ids = jax.random.randint(key_list[1], (NUM_STEPS, BATCH), 0, VOCAB, dtype=jnp.int32)
    base_lens = jax.random.randint(key_list[2], (BATCH,), 0, CACHE_LEN - 1, dtype=jnp.int32)
    perm_order = jax.random.permutation(key_list[3], BATCH)
    seq_lens = base_lens.at[perm_order[0]].set(CACHE_LEN - 2).at[perm_order[1]].set(0)
    embed = jax.random.normal(key_list[4], (VOCAB, D), jnp.float32).astype(jnp.bfloat16)
    ln_gain = (1.0 + 0.3 * jax.random.normal(key_list[5], (D,), jnp.float32)).astype(jnp.bfloat16)
    w_in = (jax.random.normal(key_list[6], (D, IN_WIDTH), jnp.float32) * D ** -0.5).astype(jnp.bfloat16)
    row_scale = jnp.where(jnp.arange(OUT_WIDTH) % OUT_DEV < ATTN_DEV, 2.0 * ATTN_WIDTH ** -0.5, FF ** -0.5)
    w_out = (jax.random.normal(key_list[7], (OUT_WIDTH, D), jnp.float32) * row_scale[:, None]).astype(jnp.bfloat16)
    final_gain = (1.6 * (1.0 + 0.3 * jax.random.normal(key_list[8], (D,), jnp.float32))).astype(jnp.bfloat16)
    k_cache = jax.random.normal(key_list[9], (BATCH, CACHE_LEN, HEAD), jnp.float32).astype(jnp.bfloat16)
    v_cache = jax.random.normal(key_list[10], (BATCH, CACHE_LEN, HEAD), jnp.float32).astype(jnp.bfloat16)
    return {'tok_ids': tok_ids, 'next_ids': next_ids, 'seq_lens': seq_lens, 'embed': embed, 'ln_gain': ln_gain, 'w_in': w_in, 'w_out': w_out, 'final_gain': final_gain, 'k_cache': k_cache, 'v_cache': v_cache}


def layer_norm(values, gain_vec):
    centered = values.astype(jnp.float32)
    centered = centered - jnp.mean(centered, axis=-1, keepdims=True)
    variance = jnp.mean(jnp.square(centered), axis=-1, keepdims=True)
    scaled = centered * lax.rsqrt(variance + NORM_EPS) * gain_vec.astype(jnp.float32)
    return scaled.astype(jnp.bfloat16)


def rotary(vectors, positions):
    half_dim = vectors.shape[-1] // 2
    inv_freq = ROPE_BASE ** (-jnp.arange(half_dim, dtype=jnp.float32) / half_dim)
    angles = positions.astype(jnp.float32)[..., None] * inv_freq
    cosine = jnp.cos(angles)
    sine_val = jnp.sin(angles)
    first_half = vectors[..., :half_dim]
    second_half = vectors[..., half_dim:]
    return jnp.concatenate([first_half * cosine - second_half * sine_val, second_half * cosine + first_half * sine_val], axis=-1)


def block_steps(tok_blk, next_blk, len_blk, k_blk, v_blk, embed, ln_gain, w_in, w_out, final_gain):
    row_count = len_blk.shape[0]
    time_ids = jnp.arange(CACHE_LEN)
    step_logp = []
    for step_idx in range(NUM_STEPS):
        positions = len_blk + step_idx
        x_rows = embed[tok_blk[step_idx]]
        normed = layer_norm(x_rows, ln_gain)
        proj_out = jnp.dot(normed, w_in, preferred_element_type=jnp.float32).astype(jnp.bfloat16)
        proj_out = proj_out.reshape(row_count, GROUP, IN_DEV)
        qkv_vec = proj_out[:, :, :QKV_DEV].reshape(row_count, QKV_WIDTH)
        gate_proj = proj_out[:, :, QKV_DEV:QKV_DEV + FF_DEV].astype(jnp.float32)
        up_proj = proj_out[:, :, QKV_DEV + FF_DEV:].astype(jnp.float32)
        mlp_act = (jax.nn.silu(gate_proj) * up_proj).astype(jnp.bfloat16)
        queries = qkv_vec[:, :ATTN_WIDTH].reshape(row_count, HEADS, HEAD).astype(jnp.float32)
        q_rot = (rotary(queries, positions[:, None]) * HEAD ** -0.5).astype(jnp.bfloat16)
        k_new = rotary(qkv_vec[:, ATTN_WIDTH:ATTN_WIDTH + HEAD].astype(jnp.float32), positions).astype(jnp.bfloat16)
        v_new = qkv_vec[:, ATTN_WIDTH + HEAD:]
        write_mask = time_ids[None, :, None] == positions[:, None, None]
        k_blk = jnp.where(write_mask, k_new[:, None, :], k_blk)
        v_blk = jnp.where(write_mask, v_new[:, None, :], v_blk)
        scores = jnp.einsum('bhd,btd->bht', q_rot.astype(jnp.float32), k_blk.astype(jnp.float32))
        visible = time_ids[None, None, :] <= positions[:, None, None]
        attn_probs = jax.nn.softmax(jnp.where(visible, scores, -jnp.inf), axis=-1).astype(jnp.bfloat16)
        attn_out = jnp.einsum('bht,btd->bhd', attn_probs.astype(jnp.float32), v_blk.astype(jnp.float32)).astype(jnp.bfloat16)
        attn_grp = attn_out.reshape(row_count, GROUP, ATTN_DEV)
        combined = jnp.concatenate([attn_grp, mlp_act], axis=2).reshape(row_count, OUT_WIDTH)
        layer_out = jnp.dot(combined, w_out, preferred_element_type=jnp.float32).astype(jnp.bfloat16)
        resid_sum = x_rows.astype(jnp.float32) + layer_out.astype(jnp.float32)
        final_normed = layer_norm(resid_sum, final_gain)
        logits = jnp.dot(final_normed, embed.T, preferred_element_type=jnp.float32) * D ** -0.5
        picked = jnp.take_along_axis(logits, next_blk[step_idx][:, None], axis=1)[:, 0]
        step_logp.append(picked - jax.nn.logsumexp(logits, axis=1))
    return jnp.stack(step_logp), k_blk, v_blk


def reference(tok_ids, next_ids, seq_lens, embed, ln_gain, w_in, w_out, final_gain, k_cache, v_cache):
    tok_grp = tok_ids.reshape(NUM_STEPS, MAP_COUNT, MAP_ROWS).transpose(1, 0, 2)
    next_grp = next_ids.reshape(NUM_STEPS, MAP_COUNT, MAP_ROWS).transpose(1, 0, 2)
    len_grp = seq_lens.reshape(MAP_COUNT, MAP_ROWS)
    k_grp = k_cache.reshape(MAP_COUNT, MAP_ROWS, CACHE_LEN, HEAD)
    v_grp = v_cache.reshape(MAP_COUNT, MAP_ROWS, CACHE_LEN, HEAD)

    def run_group(group_in):
        return block_steps(group_in[0], group_in[1], group_in[2], group_in[3], group_in[4], embed, ln_gain, w_in, w_out, final_gain)

    logp_grp, k_done, v_done = lax.map(run_group, (tok_grp, next_grp, len_grp, k_grp, v_grp))
    log_probs = logp_grp.transpose(1, 0, 2).reshape(NUM_STEPS, BATCH)
    return log_probs, k_done.reshape(BATCH, CACHE_LEN, HEAD), v_done.reshape(BATCH, CACHE_LEN, HEAD)
```

```python
import functools

import jax
import jax.numpy as jnp
from jax import lax
from jax.experimental import pallas as pl
from jax.experimental.pallas import tpu as pltpu
from jax.sharding import PartitionSpec as P

ROPE_BASE = 10000.0
NORM_EPS = 1e-6
MESH_ID = pl.DeviceIdType.MESH
ROWS = 16
NZ = 4
NDEV = 32
STEPS = 2
RS_SPLIT = 2
AG_SPLIT = 1
BF16 = jnp.bfloat16
F32 = jnp.float32


def rotary(vectors, positions):
    half_dim = vectors.shape[-1] // 2
    inv_freq = ROPE_BASE ** (-jnp.arange(half_dim, dtype=jnp.float32) / half_dim)
    angles = positions.astype(jnp.float32)[..., None] * inv_freq
    cosine = jnp.cos(angles)
    sine_val = jnp.sin(angles)
    first_half = vectors[..., :half_dim]
    second_half = vectors[..., half_dim:]
    return jnp.concatenate([first_half * cosine - second_half * sine_val, second_half * cosine + first_half * sine_val], axis=-1)


def norm_rows(values, gain):
    centered = values - jnp.mean(values, axis=-1, keepdims=True)
    variance = jnp.mean(jnp.square(centered), axis=-1, keepdims=True)
    return (centered * lax.rsqrt(variance + NORM_EPS) * gain).astype(BF16)


def dot_nt(a, b):
    return lax.dot_general(a, b, (((1,), (1,)), ((), ())), preferred_element_type=F32)


class Place:
    def __init__(self):
        self.me = lax.axis_index("tp")
        self.c = lax.rem(self.me, 2)
        self.x = lax.rem(lax.div(self.me, 2), 2)
        self.y = lax.rem(lax.div(self.me, 4), 2)
        self.z = lax.div(self.me, 8)
        self.sib = self.me + 1 - 2 * self.c
        self.xpeer = self.me + 2 * (1 - 2 * self.x)
        self.ypeer = self.me + 4 * (1 - 2 * self.y)

    def zpeer(self, k):
        return lax.rem(self.me + 8 * k, NDEV)

    def peer(self, k):
        return lax.rem(self.me + k, NDEV)


def remote(src, dst, ssem, rsem, dev):
    return pltpu.make_async_remote_copy(src_ref=src, dst_ref=dst, send_sem=ssem, recv_sem=rsem, device_id=(dev,), device_id_type=MESH_ID)


def greet(place):
    barrier = pltpu.get_barrier_semaphore()

    def body(k, _):
        pl.semaphore_signal(barrier, inc=1, device_id=(place.peer(k),), device_id_type=MESH_ID)
        return 0

    lax.fori_loop(1, NDEV, body, 0)
    return barrier


def exchange_scratch(width):
    w = width // RS_SPLIT
    return dict(
        part=pltpu.VMEM((STEPS, NZ, 2, 2, 2, ROWS, width), BF16),
        rc=pltpu.VMEM((STEPS, NZ, 2, 2, ROWS, width), BF16),
        s1=pltpu.VMEM((STEPS, NZ, 2, 2, ROWS, width), BF16),
        r1a=pltpu.VMEM((STEPS, RS_SPLIT, NZ, 2, ROWS, w // 2), BF16),
        r1b=pltpu.VMEM((STEPS, RS_SPLIT, NZ, 2, ROWS, w // 2), BF16),
        s2a=pltpu.VMEM((STEPS, RS_SPLIT, NZ, 2, ROWS, w // 2), BF16),
        s2b=pltpu.VMEM((STEPS, RS_SPLIT, NZ, 2, ROWS, w // 2), BF16),
        r2a=pltpu.VMEM((STEPS, RS_SPLIT, NZ, ROWS, w // 2), BF16),
        r2b=pltpu.VMEM((STEPS, RS_SPLIT, NZ, ROWS, w // 2), BF16),
        s3=pltpu.VMEM((STEPS, RS_SPLIT, NZ, ROWS, w), BF16),
        r3=pltpu.VMEM((STEPS, RS_SPLIT, NZ - 1, ROWS, w), BF16),
        tot=pltpu.VMEM((STEPS, ROWS, width), F32),
        full=pltpu.VMEM((STEPS, NZ, 2, 2, 2, ROWS, width), BF16),
        rs_s=pltpu.SemaphoreType.DMA((STEPS * RS_SPLIT, 8)),
        rs_r=pltpu.SemaphoreType.DMA((STEPS * RS_SPLIT, 8)),
        ag_s=pltpu.SemaphoreType.DMA((STEPS * AG_SPLIT, 8)),
        ag_r=pltpu.SemaphoreType.DMA((STEPS * AG_SPLIT, 8)),
    )


EXCHANGE_NAMES = ("part", "rc", "s1", "r1a", "r1b", "s2a", "s2b", "r2a", "r2b", "s3", "r3", "tot", "full", "rs_s", "rs_r", "ag_s", "ag_r")


def run_exchange(place, b, width, produce, barrier_wait, finalize, consume):
    x, y, z, c = place.x, place.y, place.z, place.c
    sent = []

    def add(dst, left, right):
        dst[...] = (left[...].astype(F32) + right[...].astype(F32)).astype(BF16)

    def rs_stages(s, h):
        w = width // RS_SPLIT
        lo = h * w
        cols = pl.ds(lo, w)
        ca, cb = pl.ds(lo, w // 2), pl.ds(lo + w // 2, w // 2)
        n = s * RS_SPLIT + h
        ss, rs = b["rs_s"], b["rs_r"]
        live = {}

        def go(j, src, dst, dev):
            cp = remote(src, dst, ss.at[n, j], rs.at[n, j], dev)
            cp.start()
            live[j] = cp
            sent.append(cp)

        def st0():
            produce(s, h)
            barrier_wait()
            go(0, b["part"].at[s, :, :, :, 1 - c, :, cols], b["rc"].at[s, :, :, :, :, cols], place.sib)

        def st1():
            live[0].wait_recv()

            def body(i, _):
                add(b["s1"].at[s, i, :, :, :, cols], b["part"].at[s, i, :, :, c, :, cols], b["rc"].at[s, i, :, :, :, cols])
                return 0

            lax.fori_loop(0, NZ, body, 0)
            go(1, b["s1"].at[s, :, :, 1 - x, :, ca], b["r1a"].at[s, h], place.xpeer)
            go(2, b["s1"].at[s, :, 1 - y, :, :, cb], b["r1b"].at[s, h], place.ypeer)

        def st2():
            live[1].wait_recv()

            def body_a(i, _):
                add(b["s2a"].at[s, h, i], b["s1"].at[s, i, :, x, :, ca], b["r1a"].at[s, h, i])
                return 0

            lax.fori_loop(0, NZ, body_a, 0)
            go(3, b["s2a"].at[s, h, :, 1 - y], b["r2a"].at[s, h], place.ypeer)
            live[2].wait_recv()

            def body_b(i, _):
                add(b["s2b"].at[s, h, i], b["s1"].at[s, i, y, :, :, cb], b["r1b"].at[s, h, i])
                return 0

            lax.fori_loop(0, NZ, body_b, 0)
            go(4, b["s2b"].at[s, h, :, 1 - x], b["r2b"].at[s, h], place.xpeer)

        def st3():
            live[3].wait_recv()
            add(b["s3"].at[s, h, :, :, pl.ds(0, w // 2)], b["s2a"].at[s, h, :, y], b["r2a"].at[s, h])
            live[4].wait_recv()
            add(b["s3"].at[s, h, :, :, pl.ds(w // 2, w // 2)], b["s2b"].at[s, h, :, x], b["r2b"].at[s, h])
            for k in range(1, NZ):
                go(4 + k, b["s3"].at[s, h, lax.rem(z + k, NZ)], b["r3"].at[s, h, k - 1], place.zpeer(k))

        def st4():
            for k in range(1, NZ):
                live[4 + k].wait_recv()
            total = b["s3"][s, h, z].astype(F32)
            for k in range(1, NZ):
                total = total + b["r3"][s, h, k - 1].astype(F32)
            b["tot"][s, :, cols] = total

        return [st0, st1, st2, st3, st4]

    def ag_stages(s, h):
        w = width // AG_SPLIT
        lo = h * w
        cols = pl.ds(lo, w)
        ca, cb = pl.ds(lo, w // 2), pl.ds(lo + w // 2, w // 2)
        n = s * AG_SPLIT + h
        ss, rs = b["ag_s"], b["ag_r"]
        full = b["full"]
        live = {}

        def go(j, ref, dev):
            cp = remote(ref, ref, ss.at[n, j], rs.at[n, j], dev)
            cp.start()
            live[j] = cp
            sent.append(cp)

        def st0():
            if h == 0:
                finalize(s)
            for k in range(1, NZ):
                go(k - 1, full.at[s, z, y, x, c, :, cols], place.zpeer(k))

        def st1():
            for k in range(1, NZ):
                live[k - 1].wait_recv()
            go(3, full.at[s, :, y, x, c, :, ca], place.ypeer)
            go(4, full.at[s, :, y, x, c, :, cb], place.xpeer)

        def st2():
            live[3].wait_recv()
            go(5, full.at[s, :, :, x, c, :, ca], place.xpeer)
            live[4].wait_recv()
            go(6, full.at[s, :, y, :, c, :, cb], place.ypeer)

        def st3():
            live[5].wait_recv()
            live[6].wait_recv()
            go(7, full.at[s, :, :, :, c, :, cols], place.sib)

        def st4():
            live[7].wait_recv()
            if h == AG_SPLIT - 1:
                consume(s)

        return [st0, st1, st2, st3, st4]

    items = []
    for s in range(STEPS):
        for h in range(RS_SPLIT):
            k = s * RS_SPLIT + h
            for t, stage in enumerate(rs_stages(s, h)):
                items.append((k + t, k, stage))
        for h in range(AG_SPLIT):
            first = s * RS_SPLIT + RS_SPLIT - 1 + 4
            for t, stage in enumerate(ag_stages(s, h)):
                items.append((first + t, 0.5 + s * RS_SPLIT + RS_SPLIT - 1 + h * 0.1, stage))
    for _, _, stage in sorted(items, key=lambda e: (e[0], e[1])):
        stage()
    for cp in sent:
        cp.wait_send()


def front_kernel(vocab_dev, width, qkv_dev, ff_dev, tok_ref, gain_ref, embed_ref, w_ref, x_ref, qkv_ref, mlp_ref,
                 emb, hot, wq, wg, wu, sq, rq, local_sem, a_s, a_r, *bufs):
    b = dict(zip(EXCHANGE_NAMES, bufs))
    place = Place()
    me = place.me
    barrier = greet(place)
    half = width // RS_SPLIT
    loads = []
    for h in range(RS_SPLIT):
        cols = pl.ds(h * half, half)
        loads.append(pltpu.make_async_copy(embed_ref.at[:, cols], emb.at[:, cols], local_sem.at[h]))
    pieces = ((wq, 0, qkv_dev), (wg, qkv_dev, ff_dev), (wu, qkv_dev + ff_dev, ff_dev))
    for i, (dst, start, size) in enumerate(pieces):
        loads.append(pltpu.make_async_copy(w_ref.at[pl.ds(start, size), :], dst, local_sem.at[RS_SPLIT + i]))
    for cp in loads:
        cp.start()
    vocab_start = me * vocab_dev

    def produce(s, h):
        if s == 0:
            loads[h].wait()
        if h == 0:
            def build(i, _):
                rows = pl.ds(pl.multiple_of(i * 128, 128), 128)
                ids = tok_ref[rows, s:s + 1] - vocab_start
                lanes = lax.broadcasted_iota(jnp.int32, (128, vocab_dev), 1)
                hot[s, rows, :] = jnp.where(ids == lanes, 1.0, 0.0).astype(BF16)
                return 0

            lax.fori_loop(0, 4, build, 0)

        tile = 512
        per = half // tile

        def mul(i, _):
            zi, ni = lax.div(i, per), lax.rem(i, per)
            rows = pl.ds(pl.multiple_of(zi * 256, 256), 256)
            cols = pl.ds(pl.multiple_of(h * half + ni * tile, tile), tile)
            out = jnp.dot(hot[s, rows, :], emb[:, cols], preferred_element_type=F32).astype(BF16)
            b["part"][s, pl.ds(2 * zi, 2), :, :, :, :, cols] = out.reshape(2, 2, 2, 2, ROWS, tile)
            return 0

        lax.fori_loop(0, 2 * per, mul, 0)

    pending = [True]

    def barrier_wait():
        if pending[0]:
            pl.semaphore_wait(barrier, NDEV - 1)
            pending[0] = False

    def finalize(s):
        rows = b["tot"][s]
        x_ref[s] = rows.astype(BF16)
        b["full"][s, place.z, place.y, place.x, place.c] = norm_rows(rows, gain_ref[...].astype(F32))

    def send_qkv(s, k):
        to = place.peer(k)
        return remote(sq.at[s, to], rq.at[me, s], a_s.at[s, k], a_r.at[s, k], to)

    def consume(s):
        if s == 0:
            for cp in loads[RS_SPLIT:]:
                cp.wait()

        def mul(i, _):
            hid = b["full"][s, pl.ds(2 * i, 2)].reshape(256, width)
            qkv = dot_nt(hid, wq[...]).astype(BF16)
            sq[s, pl.ds(16 * i, 16)] = qkv.reshape(16, ROWS, qkv_dev)
            return 0

        lax.fori_loop(0, 2, mul, 0)
        rq[me, s] = sq[s, me]

        def send(k, _):
            send_qkv(s, k).start()
            return 0

        lax.fori_loop(1, NDEV, send, 0)

        def mlp(i, _):
            hid = b["full"][s, pl.ds(2 * i, 2)].reshape(256, width)
            gate = dot_nt(hid, wg[...]).astype(BF16).astype(F32)
            up = dot_nt(hid, wu[...]).astype(BF16).astype(F32)
            act = (gate * (1.0 / (1.0 + jnp.exp(-gate)))) * up
            mlp_ref[s, pl.ds(pl.multiple_of(256 * i, 256), 256), :] = act.astype(BF16)
            return 0

        lax.fori_loop(0, 2, mlp, 0)

    run_exchange(place, b, width, produce, barrier_wait, finalize, consume)
    for s in range(STEPS):
        def finish(k, _):
            cp = send_qkv(s, k)
            cp.wait_send()
            cp.wait_recv()
            return 0

        lax.fori_loop(1, NDEV, finish, 0)

    def copy_out(i, _):
        qkv_ref[i] = rq[i]
        return 0

    lax.fori_loop(0, NDEV, copy_out, 0)


def back_kernel(vocab_dev, width, attn_dev, ff_dev, scale, send_ref, mlp_ref, x_ref, gain_ref, next_ref, w_ref, embed_ref, out_ref,
                emb, wv, ac, r8, r4, local_sem, a_s, a_r, st_s, st_r, *bufs):
    b = dict(zip(EXCHANGE_NAMES, bufs))
    place = Place()
    me = place.me
    r8[...] = jnp.zeros_like(r8)
    r4[...] = jnp.zeros_like(r4)
    barrier = greet(place)
    load_w = pltpu.make_async_copy(w_ref, wv, local_sem.at[0])
    load_e = pltpu.make_async_copy(embed_ref, emb, local_sem.at[1])
    load_w.start()
    load_e.start()
    vocab_start = me * vocab_dev
    half = width // RS_SPLIT

    def send_attn(k):
        to = place.peer(k)
        return remote(send_ref.at[to], ac.at[:, me], a_s.at[k], a_r.at[k], to)

    ac[:, me] = send_ref[me]
    pl.semaphore_wait(barrier, NDEV - 1)

    def send(k, _):
        send_attn(k).start()
        return 0

    lax.fori_loop(1, NDEV, send, 0)
    load_w.wait()

    def arrive(k, _):
        send_attn(k).wait_recv()
        return 0

    lax.fori_loop(1, NDEV, arrive, 0)

    def produce(s, h):
        tile = 512
        per = half // tile

        def mul(i, _):
            zi, ni = lax.div(i, per), lax.rem(i, per)
            cols = pl.ds(pl.multiple_of(h * half + ni * tile, tile), tile)
            att = ac[s, pl.ds(16 * zi, 16)].reshape(256, attn_dev)
            mid = mlp_ref[s, pl.ds(pl.multiple_of(256 * zi, 256), 256), :]
            out = jnp.dot(att, wv[0:attn_dev, cols], preferred_element_type=F32)
            out = out + jnp.dot(mid, wv[attn_dev:attn_dev + ff_dev, cols], preferred_element_type=F32)
            b["part"][s, pl.ds(2 * zi, 2), :, :, :, :, cols] = out.astype(BF16).reshape(2, 2, 2, 2, ROWS, tile)
            return 0

        lax.fori_loop(0, 2 * per, mul, 0)

    def finalize(s):
        layer = b["tot"][s].astype(BF16).astype(F32)
        resid = x_ref[s].astype(F32) + layer
        b["full"][s, place.z, place.y, place.x, place.c] = norm_rows(resid, gain_ref[...].astype(F32))

    plane = lax.rem(me, 8)

    def send_plane(s, k):
        q = lax.rem(plane + k, 8)
        return remote(r8.at[s, plane], r8.at[s, plane], st_s.at[s, k], st_r.at[s, k], me - plane + q)

    def send_line(s, k):
        return remote(r4.at[s, place.z], r4.at[s, place.z], st_s.at[s, 8 + k], st_r.at[s, 8 + k], place.zpeer(k))

    def consume(s):
        if s == 0:
            load_e.wait()
        batch = NDEV * ROWS
        tile = 256
        nxt = next_ref[s] - vocab_start

        def mul(i, carry):
            top, den, hit = carry
            rows = pl.ds(pl.multiple_of(i * tile, tile), tile)
            zed = b["full"][s].reshape(batch, width)
            logits = dot_nt(emb[rows, :], zed) * scale
            new = jnp.maximum(top, jnp.max(logits, axis=0, keepdims=True))
            den = den * jnp.exp(top - new) + jnp.sum(jnp.exp(logits - new), axis=0, keepdims=True)
            ids = lax.broadcasted_iota(jnp.int32, (tile, batch), 0) + i * tile
            hit = hit + jnp.sum(jnp.where(ids == nxt, logits, 0.0), axis=0, keepdims=True)
            return new, den, hit

        zero = jnp.zeros((1, batch), F32)
        top, den, hit = lax.fori_loop(0, vocab_dev // tile, mul, (jnp.full((1, batch), -jnp.inf, F32), zero, zero))
        r8[s, plane, 0:1, :] = top
        r8[s, plane, 1:2, :] = den
        r8[s, plane, 2:3, :] = hit
        for k in range(1, 8):
            send_plane(s, k).start()

    def merge(buf, s, count):
        top = buf[s, 0, 0:1, :]
        for i in range(1, count):
            top = jnp.maximum(top, buf[s, i, 0:1, :])
        den = jnp.zeros_like(top)
        hit = jnp.zeros_like(top)
        for i in range(count):
            den = den + buf[s, i, 1:2, :] * jnp.exp(buf[s, i, 0:1, :] - top)
            hit = hit + buf[s, i, 2:3, :]
        return top, den, hit

    run_exchange(place, b, width, produce, lambda: None, finalize, consume)
    for s in range(STEPS):
        for k in range(1, 8):
            send_plane(s, k).wait_recv()
        top, den, hit = merge(r8, s, 8)
        r4[s, place.z, 0:1, :] = top
        r4[s, place.z, 1:2, :] = den
        r4[s, place.z, 2:3, :] = hit
        for k in range(1, NZ):
            send_line(s, k).start()
    for s in range(STEPS):
        for k in range(1, NZ):
            send_line(s, k).wait_recv()
        top, den, hit = merge(r4, s, NZ)
        out_ref[s] = hit - top - jnp.log(den)
    for s in range(STEPS):
        for k in range(1, 8):
            send_plane(s, k).wait_send()
        for k in range(1, NZ):
            send_line(s, k).wait_send()

    def finish(k, _):
        send_attn(k).wait_send()
        return 0

    lax.fori_loop(1, NDEV, finish, 0)


def attention_kernel(heads, lens_ref, q_ref, kn_ref, vn_ref, kc_ref, vc_ref, o_ref, ko_ref, vo_ref):
    first = lens_ref[pl.program_id(0)]
    ko_ref[...] = kc_ref[...]
    vo_ref[...] = vc_ref[...]
    for s in range(STEPS):
        pos = first + s
        base = pl.multiple_of(lax.div(pos, 16) * 16, 16)
        rows = lax.broadcasted_iota(jnp.int32, (16, ko_ref.shape[2]), 0) == pos - base
        ko_ref[0, pl.ds(base, 16), :] = jnp.where(rows, kn_ref[0, s:s + 1, :], ko_ref[0, pl.ds(base, 16), :])
        vo_ref[0, pl.ds(base, 16), :] = jnp.where(rows, vn_ref[0, s:s + 1, :], vo_ref[0, pl.ds(base, 16), :])
    scores = dot_nt(q_ref[0], ko_ref[0])
    times = lax.broadcasted_iota(jnp.int32, scores.shape, 1)
    limit = first + jnp.where(lax.broadcasted_iota(jnp.int32, scores.shape, 0) >= heads, 1, 0)
    scores = jnp.where(times <= limit, scores, -jnp.inf)
    scores = jnp.exp(scores - jnp.max(scores, axis=1, keepdims=True))
    probs = (scores / jnp.sum(scores, axis=1, keepdims=True)).astype(BF16)
    o_ref[0] = jnp.dot(probs, vo_ref[0], preferred_element_type=F32).astype(BF16)


def solution(mesh):
    def device_fn(tok_ids, next_ids, seq_lens, embed_loc, ln_gain, w_in_loc, w_out_loc, final_gain, k_loc, v_loc):
        steps, batch = tok_ids.shape
        vocab_dev, width = embed_loc.shape
        batch_dev, cache_len, head_dim = k_loc.shape
        in_dev, out_dev = w_in_loc.shape[1], w_out_loc.shape[0]
        kv_dev = 2 * head_dim // NDEV
        attn_dev = 2 * out_dev - in_dev + kv_dev
        ff_dev = out_dev - attn_dev
        qkv_dev = attn_dev + kv_dev
        attn_width = attn_dev * NDEV
        heads = attn_width // head_dim
        dev_index = lax.axis_index('tp')
        own_lens = lax.dynamic_slice_in_dim(seq_lens, dev_index * batch_dev, batch_dev)

        scratch = exchange_scratch(width)
        exchange = [scratch[name] for name in EXCHANGE_NAMES]
        vmem = pl.BlockSpec(memory_space=pltpu.VMEM)
        anym = pl.BlockSpec(memory_space=pl.ANY)
        dma = pltpu.SemaphoreType.DMA
        x_own, qkv_parts, mlp = pl.pallas_call(
            functools.partial(front_kernel, vocab_dev, width, qkv_dev, ff_dev),
            out_shape=(
                jax.ShapeDtypeStruct((steps, batch_dev, width), BF16),
                jax.ShapeDtypeStruct((NDEV, steps, batch_dev, qkv_dev), BF16),
                jax.ShapeDtypeStruct((steps, batch, ff_dev), BF16),
            ),
            in_specs=[vmem, vmem, anym, anym],
            out_specs=(vmem, vmem, vmem),
            scratch_shapes=[
                pltpu.VMEM((vocab_dev, width), BF16),
                pltpu.VMEM((steps, batch, vocab_dev), BF16),
                pltpu.VMEM((qkv_dev, width), BF16),
                pltpu.VMEM((ff_dev, width), BF16),
                pltpu.VMEM((ff_dev, width), BF16),
                pltpu.VMEM((steps, NDEV, batch_dev, qkv_dev), BF16),
                pltpu.VMEM((NDEV, steps, batch_dev, qkv_dev), BF16),
                dma((RS_SPLIT + 3,)),
                dma((steps, NDEV)),
                dma((steps, NDEV)),
            ] + exchange,
            compiler_params=pltpu.CompilerParams(collective_id=0, has_side_effects=True, vmem_limit_bytes=60 * 1024 * 1024),
            name="front",
        )(tok_ids.T, ln_gain.reshape(1, width), embed_loc, w_in_loc.T)

        qkv_own = qkv_parts.transpose(1, 2, 0, 3).reshape(steps, batch_dev, NDEV * qkv_dev)
        positions = own_lens[None, :] + jnp.arange(steps, dtype=own_lens.dtype)[:, None]
        queries = qkv_own[..., :attn_width].reshape(steps, batch_dev, heads, head_dim).astype(F32)
        q_rot = (rotary(queries, positions[..., None]) * head_dim ** -0.5).astype(BF16)
        q_rot = q_rot.transpose(1, 0, 2, 3).reshape(batch_dev, steps * heads, head_dim)
        k_new = rotary(qkv_own[..., attn_width:attn_width + head_dim].astype(F32), positions).astype(BF16).transpose(1, 0, 2)
        v_new = qkv_own[..., attn_width + head_dim:].transpose(1, 0, 2)

        def row(i, lens):
            return (i, 0, 0)

        cache_spec = pl.BlockSpec((1, cache_len, head_dim), row)
        attn, k_out, v_out = pl.pallas_call(
            functools.partial(attention_kernel, heads),
            out_shape=(
                jax.ShapeDtypeStruct((batch_dev, steps * heads, head_dim), BF16),
                jax.ShapeDtypeStruct(k_loc.shape, BF16),
                jax.ShapeDtypeStruct(v_loc.shape, BF16),
            ),
            grid_spec=pltpu.PrefetchScalarGridSpec(
                num_scalar_prefetch=1,
                grid=(batch_dev,),
                in_specs=[
                    pl.BlockSpec((1, steps * heads, head_dim), row),
                    pl.BlockSpec((1, steps, head_dim), row),
                    pl.BlockSpec((1, steps, head_dim), row),
                    cache_spec,
                    cache_spec,
                ],
                out_specs=(pl.BlockSpec((1, steps * heads, head_dim), row), cache_spec, cache_spec),
            ),
            compiler_params=pltpu.CompilerParams(vmem_limit_bytes=32 * 1024 * 1024),
            name="attention",
        )(own_lens, q_rot, k_new, v_new, k_loc, v_loc)

        attn_send = attn.reshape(batch_dev, steps, NDEV, attn_dev).transpose(2, 1, 0, 3)
        log_probs = pl.pallas_call(
            functools.partial(back_kernel, vocab_dev, width, attn_dev, ff_dev, width ** -0.5),
            out_shape=jax.ShapeDtypeStruct((steps, 1, batch), F32),
            in_specs=[vmem, vmem, vmem, vmem, vmem, anym, anym],
            out_specs=vmem,
            scratch_shapes=[
                pltpu.VMEM((vocab_dev, width), BF16),
                pltpu.VMEM((out_dev, width), BF16),
                pltpu.VMEM((steps, NDEV, batch_dev, attn_dev), BF16),
                pltpu.VMEM((steps, 8, 8, batch), F32),
                pltpu.VMEM((steps, NZ, 8, batch), F32),
                dma((2,)),
                dma((NDEV,)),
                dma((NDEV,)),
                dma((steps, 12)),
                dma((steps, 12)),
            ] + exchange,
            compiler_params=pltpu.CompilerParams(collective_id=1, has_side_effects=True, vmem_limit_bytes=60 * 1024 * 1024),
            name="back",
        )(attn_send, mlp, x_own, final_gain.reshape(1, width), next_ids.reshape(steps, 1, batch), w_out_loc, embed_loc)
        return log_probs.reshape(steps, batch), k_out, v_out

    cache_spec = P('tp', None, None)
    return jax.shard_map(device_fn, mesh=mesh, in_specs=(P(), P(), P(), P('tp', None), P(), P(None, 'tp'), P('tp', None), P(), cache_spec, cache_spec), out_specs=(P(), cache_spec, cache_spec), check_vma=False)
```

```python
import functools

import jax
import jax.numpy as jnp
from jax import lax
from jax.experimental import pallas as pl
from jax.experimental.pallas import tpu as pltpu
from jax.sharding import PartitionSpec as P

ROPE_BASE = 10000.0
NORM_EPS = 1e-6
MESH_ID = pl.DeviceIdType.MESH
ROWS = 8
NZ = 4
NDEV = 32
STEPS = 2
HALVES = 2
PIECES = STEPS * HALVES
FRONT_ORDER = (
    "r00 r10 r01 r11 r20 r30 r02 r12 r21 r03 r13 r31 r04 r22 g00 r14 g10 r32 r23 g01 "
    "r33 g11 r24 g20 g12 g02 r34 g30 g21 g03 g31 g13 g22 g32 g04 g14 g23 g24 g33 g34"
)
BACK_ORDER = (
    "r00 r01 r10 r11 r20 r30 r02 r12 r21 r31 r03 r13 r04 g00 r32 r14 g10 r22 r33 g01 "
    "g11 r23 g02 r34 g30 r24 g20 g12 g03 g31 g21 g13 g32 g04 g22 g33 g14 g23 g34 g24"
)
KERNEL_VMEM = 60 * 1024 * 1024
BF16 = jnp.bfloat16
F32 = jnp.float32


def rotary(vectors, positions):
    half_dim = vectors.shape[-1] // 2
    inv_freq = ROPE_BASE ** (-jnp.arange(half_dim, dtype=jnp.float32) / half_dim)
    angles = positions.astype(jnp.float32)[..., None] * inv_freq
    cosine = jnp.cos(angles)
    sine_val = jnp.sin(angles)
    first_half = vectors[..., :half_dim]
    second_half = vectors[..., half_dim:]
    return jnp.concatenate([first_half * cosine - second_half * sine_val, second_half * cosine + first_half * sine_val], axis=-1)


def norm_rows(values, gain):
    centered = values - jnp.mean(values, axis=-1, keepdims=True)
    variance = jnp.mean(jnp.square(centered), axis=-1, keepdims=True)
    return (centered * lax.rsqrt(variance + NORM_EPS) * gain).astype(BF16)


def dot_nt(a, b):
    return lax.dot_general(a, b, (((1,), (1,)), ((), ())), preferred_element_type=F32)


class Place:
    def __init__(self):
        self.me = lax.axis_index("tp")
        self.c = lax.rem(self.me, 2)
        self.x = lax.rem(lax.div(self.me, 2), 2)
        self.y = lax.rem(lax.div(self.me, 4), 2)
        self.z = lax.div(self.me, 8)
        self.sib = self.me + 1 - 2 * self.c
        self.xpeer = self.me + 2 * (1 - 2 * self.x)
        self.ypeer = self.me + 4 * (1 - 2 * self.y)

    def zpeer(self, k):
        return lax.rem(self.me + 8 * k, NDEV)

    def peer(self, k):
        return lax.rem(self.me + k, NDEV)


def remote(src, dst, ssem, rsem, dev):
    return pltpu.make_async_remote_copy(src_ref=src, dst_ref=dst, send_sem=ssem, recv_sem=rsem, device_id=(dev,), device_id_type=MESH_ID)


def greet(place):
    barrier = pltpu.get_barrier_semaphore()

    def body(k, _):
        pl.semaphore_signal(barrier, inc=1, device_id=(place.peer(k),), device_id_type=MESH_ID)
        return 0

    lax.fori_loop(1, NDEV, body, 0)
    return barrier


def exchange_scratch(width):
    half = width // 2
    return dict(
        part=pltpu.VMEM((PIECES, NZ, 2, 2, 2, ROWS, width), BF16),
        rc=pltpu.VMEM((PIECES, NZ, 2, 2, ROWS, width), BF16),
        s1=pltpu.VMEM((PIECES, NZ, 2, 2, ROWS, width), BF16),
        r1a=pltpu.VMEM((PIECES, NZ, 2, ROWS, half), BF16),
        r1b=pltpu.VMEM((PIECES, NZ, 2, ROWS, half), BF16),
        s2a=pltpu.VMEM((PIECES, NZ, 2, ROWS, half), BF16),
        s2b=pltpu.VMEM((PIECES, NZ, 2, ROWS, half), BF16),
        r2a=pltpu.VMEM((PIECES, NZ, ROWS, half), BF16),
        r2b=pltpu.VMEM((PIECES, NZ, ROWS, half), BF16),
        s3=pltpu.VMEM((PIECES, NZ, ROWS, width), BF16),
        r3=pltpu.VMEM((PIECES, NZ - 1, ROWS, width), BF16),
        full=pltpu.VMEM((PIECES, NZ, 2, 2, 2, ROWS, width), BF16),
        rows=pltpu.VMEM((NDEV * ROWS, width), BF16),
        rs_s=pltpu.SemaphoreType.DMA((PIECES, 8)),
        rs_r=pltpu.SemaphoreType.DMA((PIECES, 8)),
        ag_s=pltpu.SemaphoreType.DMA((PIECES, 8)),
        ag_r=pltpu.SemaphoreType.DMA((PIECES, 8)),
    )


EXCHANGE_NAMES = ("part", "rc", "s1", "r1a", "r1b", "s2a", "s2b", "r2a", "r2b", "s3", "r3", "full", "rows", "rs_s", "rs_r", "ag_s", "ag_r")


def run_exchange(place, b, width, order, produce, barrier_wait, finalize, consume):
    x, y, z, c = place.x, place.y, place.z, place.c
    half = width // 2
    ca, cb = pl.ds(0, half), pl.ds(half, half)
    full = b["full"]
    sent = []

    def add(dst, left, right):
        dst[...] = (left[...].astype(F32) + right[...].astype(F32)).astype(BF16)

    def add_z(dst, left, right):
        def body(i, _):
            add(dst(i), left(i), right(i))
            return 0

        lax.fori_loop(0, NZ, body, 0)

    def rs_stages(n):
        live = {}

        def go(j, src, dst, dev):
            cp = remote(src, dst, b["rs_s"].at[n, j], b["rs_r"].at[n, j], dev)
            cp.start()
            live[j] = cp
            sent.append(cp)

        def st0():
            produce(n)
            barrier_wait()
            go(0, b["part"].at[n, :, :, :, 1 - c], b["rc"].at[n], place.sib)

        def st1():
            live[0].wait_recv()
            add_z(lambda i: b["s1"].at[n, i], lambda i: b["part"].at[n, i, :, :, c], lambda i: b["rc"].at[n, i])
            go(1, b["s1"].at[n, :, :, 1 - x, :, ca], b["r1a"].at[n], place.xpeer)
            go(2, b["s1"].at[n, :, 1 - y, :, :, cb], b["r1b"].at[n], place.ypeer)

        def st2():
            live[1].wait_recv()
            add_z(lambda i: b["s2a"].at[n, i], lambda i: b["s1"].at[n, i, :, x, :, ca], lambda i: b["r1a"].at[n, i])
            go(3, b["s2a"].at[n, :, 1 - y], b["r2a"].at[n], place.ypeer)
            live[2].wait_recv()
            add_z(lambda i: b["s2b"].at[n, i], lambda i: b["s1"].at[n, i, y, :, :, cb], lambda i: b["r1b"].at[n, i])
            go(4, b["s2b"].at[n, :, 1 - x], b["r2b"].at[n], place.xpeer)

        def st3():
            live[3].wait_recv()
            add(b["s3"].at[n, :, :, ca], b["s2a"].at[n, :, y], b["r2a"].at[n])
            live[4].wait_recv()
            add(b["s3"].at[n, :, :, cb], b["s2b"].at[n, :, x], b["r2b"].at[n])
            for k in range(1, NZ):
                go(4 + k, b["s3"].at[n, lax.rem(z + k, NZ)], b["r3"].at[n, k - 1], place.zpeer(k))

        def st4():
            for k in range(1, NZ):
                live[4 + k].wait_recv()

        return [st0, st1, st2, st3, st4]

    def ag_stages(n):
        live = {}

        def go(j, ref, dev):
            cp = remote(ref, ref, b["ag_s"].at[n, j], b["ag_r"].at[n, j], dev)
            cp.start()
            live[j] = cp
            sent.append(cp)

        def st0():
            total = b["s3"][n, z].astype(F32)
            for k in range(1, NZ):
                total = total + b["r3"][n, k - 1].astype(F32)
            full[n, z, y, x, c] = finalize(n, total)
            for k in range(1, NZ):
                go(k - 1, full.at[n, z, y, x, c], place.zpeer(k))

        def st1():
            for k in range(1, NZ):
                live[k - 1].wait_recv()
            go(3, full.at[n, :, y, x, c, :, ca], place.ypeer)
            go(4, full.at[n, :, y, x, c, :, cb], place.xpeer)

        def st2():
            live[3].wait_recv()
            go(5, full.at[n, :, :, x, c, :, ca], place.xpeer)
            live[4].wait_recv()
            go(6, full.at[n, :, y, :, c, :, cb], place.ypeer)

        def st3():
            live[5].wait_recv()
            live[6].wait_recv()
            go(7, full.at[n, :, :, :, c], place.sib)

        def st4():
            live[7].wait_recv()

            def body(i, _):
                block = full[n, i].astype(F32).reshape(8 * ROWS, width).astype(BF16)
                b["rows"][pl.ds(pl.multiple_of(i * 8 * ROWS, 8 * ROWS), 8 * ROWS), :] = block
                return 0

            lax.fori_loop(0, NZ, body, 0)
            consume(n)

        return [st0, st1, st2, st3, st4]

    stages = {"r": [rs_stages(n) for n in range(PIECES)], "g": [ag_stages(n) for n in range(PIECES)]}
    for item in order.split():
        with jax.named_scope(item):
            stages[item[0]][int(item[1])][int(item[2])]()
    for cp in sent:
        cp.wait_send()


def front_kernel(vocab_dev, width, qkv_dev, ff_dev, tok_ref, gain_ref, embed_ref, w_ref, x_ref, qkv_ref, mlp_ref,
                 emb, ids, hot, wq, wg, wu, sq, rq, local_sem, a_s, a_r, *bufs):
    b = dict(zip(EXCHANGE_NAMES, bufs))
    place = Place()
    me = place.me
    barrier = greet(place)
    batch = NDEV * HALVES * ROWS
    total = NDEV * ROWS
    tile = 512
    loads = []
    for h in range(width // tile):
        cols = pl.ds(h * tile, tile)
        loads.append(pltpu.make_async_copy(embed_ref.at[:, cols], emb.at[:, cols], local_sem.at[h]))
    pieces = ((wq, 0, qkv_dev), (wg, qkv_dev, ff_dev), (wu, qkv_dev + ff_dev, ff_dev))
    for i, (dst, start, size) in enumerate(pieces):
        loads.append(pltpu.make_async_copy(w_ref.at[pl.ds(start, size), :], dst, local_sem.at[width // tile + i]))
    for cp in loads:
        cp.start()
    vocab_start = me * vocab_dev
    for s in range(STEPS):
        row = jnp.broadcast_to((tok_ref[s:s + 1, :] - vocab_start).astype(F32), (8, batch))
        ids[s] = row.T.astype(jnp.int32).reshape(NDEV, HALVES, ROWS, 8)

    def produce(n):
        col = ids[n // HALVES, :, n % HALVES].reshape(total, 8)
        for i in range(2):
            lanes = lax.broadcasted_iota(jnp.int32, (total // 2, vocab_dev), 1)
            mine = col[i * total // 2:(i + 1) * total // 2, 0:1]
            hot[pl.ds(i * total // 2, total // 2), :] = jnp.where(mine == lanes, 1.0, 0.0).astype(BF16)
        for h in range(width // tile):
            cols = pl.ds(h * tile, tile)
            if n == 0:
                loads[h].wait()
            out = jnp.dot(hot[...], emb[:, cols], preferred_element_type=F32)
            b["part"][n, :, :, :, :, :, cols] = out.reshape(NZ, 2, 2, 2, ROWS, tile).astype(BF16)

    pending = [True]

    def barrier_wait():
        if pending[0]:
            pl.semaphore_wait(barrier, NDEV - 1)
            pending[0] = False

    def finalize(n, rows):
        x_ref[n] = rows.astype(BF16)
        return norm_rows(rows, gain_ref[...].astype(F32))

    def send_qkv(s, k):
        to = place.peer(k)
        pair = pl.ds(HALVES * s, HALVES)
        return remote(sq.at[pair, to], rq.at[me, pair], a_s.at[s, k], a_r.at[s, k], to)

    def consume(n):
        if n == 0:
            for cp in loads[width // tile:]:
                cp.wait()
        qkv = dot_nt(b["rows"][...], wq[...])
        sq[n] = qkv.reshape(NDEV, ROWS, qkv_dev).astype(BF16)
        rq[me, n] = sq[n, me]
        if n % HALVES == HALVES - 1:
            def send(k, _):
                send_qkv(n // HALVES, k).start()
                return 0

            lax.fori_loop(1, NDEV, send, 0)
        gate = dot_nt(b["rows"][...], wg[...]).astype(BF16).astype(F32)
        up = dot_nt(b["rows"][...], wu[...]).astype(BF16).astype(F32)
        mlp_ref[n] = ((gate * (1.0 / (1.0 + jnp.exp(-gate)))) * up).astype(BF16)

    run_exchange(place, b, width, FRONT_ORDER, produce, barrier_wait, finalize, consume)
    with jax.named_scope("qkv_arrive"):
        for s in range(STEPS):
            def finish(k, _):
                cp = send_qkv(s, k)
                cp.wait_send()
                cp.wait_recv()
                return 0

            lax.fori_loop(1, NDEV, finish, 0)

    with jax.named_scope("qkv_out"):
        def copy_out(i, _):
            qkv_ref[i] = rq[i]
            return 0

        lax.fori_loop(0, NDEV, copy_out, 0)


def back_kernel(vocab_dev, width, attn_dev, ff_dev, scale, send_ref, mlp_ref, x_ref, gain_ref, next_ref, w_ref, embed_ref, out_ref,
                emb, wv, ac, r8, r4, local_sem, a_s, a_r, st_s, st_r, *bufs):
    b = dict(zip(EXCHANGE_NAMES, bufs))
    place = Place()
    me = place.me
    r8[...] = jnp.zeros_like(r8)
    r4[...] = jnp.zeros_like(r4)
    barrier = greet(place)
    load_w = pltpu.make_async_copy(w_ref, wv, local_sem.at[0])
    load_e = pltpu.make_async_copy(embed_ref, emb, local_sem.at[1])
    load_w.start()
    load_e.start()
    vocab_start = me * vocab_dev
    total = NDEV * ROWS

    def send_attn(k):
        to = place.peer(k)
        return remote(send_ref.at[to], ac.at[:, me], a_s.at[k], a_r.at[k], to)

    ac[:, me] = send_ref[me]
    with jax.named_scope("barrier"):
        pl.semaphore_wait(barrier, NDEV - 1)

    def send(k, _):
        send_attn(k).start()
        return 0

    with jax.named_scope("attn_send"):
        lax.fori_loop(1, NDEV, send, 0)
        load_w.wait()

    def arrive(k, _):
        send_attn(k).wait_recv()
        return 0

    with jax.named_scope("attn_arrive"):
        lax.fori_loop(1, NDEV, arrive, 0)

    def produce(n):
        tile = 512
        att = ac[n].astype(F32).reshape(total, attn_dev).astype(BF16)

        def mul(i, _):
            cols = pl.ds(pl.multiple_of(i * tile, tile), tile)
            out = jnp.dot(att, wv[0:attn_dev, cols], preferred_element_type=F32)
            out = out + jnp.dot(mlp_ref[n], wv[attn_dev:attn_dev + ff_dev, cols], preferred_element_type=F32)
            b["part"][n, :, :, :, :, :, cols] = out.reshape(NZ, 2, 2, 2, ROWS, tile).astype(BF16)
            return 0

        lax.fori_loop(0, width // tile, mul, 0)

    def finalize(n, rows):
        resid = x_ref[n].astype(F32) + rows.astype(BF16).astype(F32)
        return norm_rows(resid, gain_ref[...].astype(F32))

    plane = lax.rem(me, 8)

    def send_plane(n, k):
        q = lax.rem(plane + k, 8)
        return remote(r8.at[n, plane], r8.at[n, plane], st_s.at[n, k], st_r.at[n, k], me - plane + q)

    def send_line(n, k):
        return remote(r4.at[n, place.z], r4.at[n, place.z], st_s.at[n, 8 + k], st_r.at[n, 8 + k], place.zpeer(k))

    def consume(n):
        if n == 0:
            load_e.wait()
        tile = 512
        nxt = next_ref[n:n + 1, :] - vocab_start

        def mul(i, carry):
            top, den, hit = carry
            rows = pl.ds(pl.multiple_of(i * tile, tile), tile)
            logits = dot_nt(emb[rows, :], b["rows"][...]) * scale
            new = jnp.maximum(top, jnp.max(logits, axis=0, keepdims=True))
            den = den * jnp.exp(top - new) + jnp.sum(jnp.exp(logits - new), axis=0, keepdims=True)
            ids = lax.broadcasted_iota(jnp.int32, (tile, total), 0) + i * tile
            hit = hit + jnp.sum(jnp.where(ids == nxt, logits, 0.0), axis=0, keepdims=True)
            return new, den, hit

        zero = jnp.zeros((1, total), F32)
        top, den, hit = lax.fori_loop(0, vocab_dev // tile, mul, (jnp.full((1, total), -jnp.inf, F32), zero, zero))
        r8[n, plane, 0:1, :] = top
        r8[n, plane, 1:2, :] = den
        r8[n, plane, 2:3, :] = hit
        for k in range(1, 8):
            send_plane(n, k).start()

    def merge(buf, n, count):
        top = buf[n, 0, 0:1, :]
        for i in range(1, count):
            top = jnp.maximum(top, buf[n, i, 0:1, :])
        den = jnp.zeros_like(top)
        hit = jnp.zeros_like(top)
        for i in range(count):
            den = den + buf[n, i, 1:2, :] * jnp.exp(buf[n, i, 0:1, :] - top)
            hit = hit + buf[n, i, 2:3, :]
        return top, den, hit

    run_exchange(place, b, width, BACK_ORDER, produce, lambda: None, finalize, consume)
    last = [int(item[1]) for item in BACK_ORDER.split() if item[0] == "g" and item[2] == "4"]
    for n in last:
        with jax.named_scope("plane"):
            for k in range(1, 8):
                send_plane(n, k).wait_recv()
            top, den, hit = merge(r8, n, 8)
            r4[n, place.z, 0:1, :] = top
            r4[n, place.z, 1:2, :] = den
            r4[n, place.z, 2:3, :] = hit
            for k in range(1, NZ):
                send_line(n, k).start()
    for n in last:
        with jax.named_scope("line"):
            for k in range(1, NZ):
                send_line(n, k).wait_recv()
            top, den, hit = merge(r4, n, NZ)
            out_ref[n:n + 1, :] = hit - top - jnp.log(den)
    for n in range(PIECES):
        for k in range(1, 8):
            send_plane(n, k).wait_send()
        for k in range(1, NZ):
            send_line(n, k).wait_send()

    def finish(k, _):
        send_attn(k).wait_send()
        return 0

    lax.fori_loop(1, NDEV, finish, 0)


def attention_kernel(heads, lens_ref, q_ref, kn_ref, vn_ref, kc_ref, vc_ref, o_ref, ko_ref, vo_ref):
    first = lens_ref[pl.program_id(0)]
    ko_ref[...] = kc_ref[...]
    vo_ref[...] = vc_ref[...]
    for s in range(STEPS):
        pos = first + s
        base = pl.multiple_of(lax.div(pos, 16) * 16, 16)
        rows = lax.broadcasted_iota(jnp.int32, (16, ko_ref.shape[2]), 0) == pos - base
        ko_ref[0, pl.ds(base, 16), :] = jnp.where(rows, kn_ref[0, s:s + 1, :], ko_ref[0, pl.ds(base, 16), :])
        vo_ref[0, pl.ds(base, 16), :] = jnp.where(rows, vn_ref[0, s:s + 1, :], vo_ref[0, pl.ds(base, 16), :])
    scores = dot_nt(q_ref[0], ko_ref[0])
    times = lax.broadcasted_iota(jnp.int32, scores.shape, 1)
    limit = first + jnp.where(lax.broadcasted_iota(jnp.int32, scores.shape, 0) >= heads, 1, 0)
    scores = jnp.where(times <= limit, scores, -jnp.inf)
    scores = jnp.exp(scores - jnp.max(scores, axis=1, keepdims=True))
    probs = (scores / jnp.sum(scores, axis=1, keepdims=True)).astype(BF16)
    o_ref[0] = jnp.dot(probs, vo_ref[0], preferred_element_type=F32).astype(BF16)


def solution(mesh):
    def device_fn(tok_ids, next_ids, seq_lens, embed_loc, ln_gain, w_in_loc, w_out_loc, final_gain, k_loc, v_loc):
        steps, batch = tok_ids.shape
        vocab_dev, width = embed_loc.shape
        batch_dev, cache_len, head_dim = k_loc.shape
        in_dev, out_dev = w_in_loc.shape[1], w_out_loc.shape[0]
        kv_dev = 2 * head_dim // NDEV
        attn_dev = 2 * out_dev - in_dev + kv_dev
        ff_dev = out_dev - attn_dev
        qkv_dev = attn_dev + kv_dev
        attn_width = attn_dev * NDEV
        heads = attn_width // head_dim
        dev_index = lax.axis_index('tp')
        own_lens = lax.dynamic_slice_in_dim(seq_lens, dev_index * batch_dev, batch_dev)

        scratch = exchange_scratch(width)
        exchange = [scratch[name] for name in EXCHANGE_NAMES]
        vmem = pl.BlockSpec(memory_space=pltpu.VMEM)
        anym = pl.BlockSpec(memory_space=pltpu.HBM)
        dma = pltpu.SemaphoreType.DMA
        pair_dims = (steps, NDEV, HALVES, ROWS)
        piece_rows = NDEV * ROWS
        x_own, qkv_parts, mlp = pl.pallas_call(
            functools.partial(front_kernel, vocab_dev, width, qkv_dev, ff_dev),
            out_shape=(
                jax.ShapeDtypeStruct((PIECES, ROWS, width), BF16),
                jax.ShapeDtypeStruct((NDEV, PIECES, ROWS, qkv_dev), BF16),
                jax.ShapeDtypeStruct((PIECES, piece_rows, ff_dev), BF16),
            ),
            in_specs=[vmem, vmem, anym, anym],
            out_specs=(vmem, vmem, vmem),
            scratch_shapes=[
                pltpu.VMEM((vocab_dev, width), BF16),
                pltpu.VMEM((steps, NDEV, HALVES, ROWS, 8), jnp.int32),
                pltpu.VMEM((piece_rows, vocab_dev), BF16),
                pltpu.VMEM((qkv_dev, width), BF16),
                pltpu.VMEM((ff_dev, width), BF16),
                pltpu.VMEM((ff_dev, width), BF16),
                pltpu.VMEM((PIECES, NDEV, ROWS, qkv_dev), BF16),
                pltpu.VMEM((NDEV, PIECES, ROWS, qkv_dev), BF16),
                dma((8,)),
                dma((steps, NDEV)),
                dma((steps, NDEV)),
            ] + exchange,
            compiler_params=pltpu.CompilerParams(collective_id=0, has_side_effects=True, vmem_limit_bytes=KERNEL_VMEM),
            cost_estimate=pl.CostEstimate(flops=40_000_000_000, bytes_accessed=8_000_000, transcendentals=0),
            name="front",
        )(tok_ids, ln_gain.reshape(1, width), embed_loc, w_in_loc.T)

        qkv_own = qkv_parts.reshape(NDEV, steps, batch_dev, qkv_dev).transpose(1, 2, 0, 3).reshape(steps, batch_dev, NDEV * qkv_dev)
        positions = own_lens[None, :] + jnp.arange(steps, dtype=own_lens.dtype)[:, None]
        queries = qkv_own[..., :attn_width].reshape(steps, batch_dev, heads, head_dim).astype(F32)
        q_rot = (rotary(queries, positions[..., None]) * head_dim ** -0.5).astype(BF16)
        q_rot = q_rot.transpose(1, 0, 2, 3).reshape(batch_dev, steps * heads, head_dim)
        k_new = rotary(qkv_own[..., attn_width:attn_width + head_dim].astype(F32), positions).astype(BF16).transpose(1, 0, 2)
        v_new = qkv_own[..., attn_width + head_dim:].transpose(1, 0, 2)

        def row(i, lens):
            return (i, 0, 0)

        cache_spec = pl.BlockSpec((1, cache_len, head_dim), row)
        attn, k_out, v_out = pl.pallas_call(
            functools.partial(attention_kernel, heads),
            out_shape=(
                jax.ShapeDtypeStruct((batch_dev, steps * heads, head_dim), BF16),
                jax.ShapeDtypeStruct(k_loc.shape, BF16),
                jax.ShapeDtypeStruct(v_loc.shape, BF16),
            ),
            grid_spec=pltpu.PrefetchScalarGridSpec(
                num_scalar_prefetch=1,
                grid=(batch_dev,),
                in_specs=[
                    pl.BlockSpec((1, steps * heads, head_dim), row),
                    pl.BlockSpec((1, steps, head_dim), row),
                    pl.BlockSpec((1, steps, head_dim), row),
                    cache_spec,
                    cache_spec,
                ],
                out_specs=(pl.BlockSpec((1, steps * heads, head_dim), row), cache_spec, cache_spec),
            ),
            compiler_params=pltpu.CompilerParams(vmem_limit_bytes=KERNEL_VMEM),
            cost_estimate=pl.CostEstimate(flops=1_000_000_000, bytes_accessed=34_000_000, transcendentals=0),
            name="attention",
        )(own_lens, q_rot, k_new, v_new, k_loc, v_loc)

        attn_send = attn.reshape(batch_dev, steps, NDEV, attn_dev).transpose(2, 1, 0, 3).reshape(NDEV, PIECES, ROWS, attn_dev)
        next_rows = next_ids.reshape(pair_dims).transpose(0, 2, 1, 3).reshape(PIECES, piece_rows)
        log_probs = pl.pallas_call(
            functools.partial(back_kernel, vocab_dev, width, attn_dev, ff_dev, width ** -0.5),
            out_shape=jax.ShapeDtypeStruct((PIECES, piece_rows), F32),
            in_specs=[vmem, vmem, vmem, vmem, vmem, anym, anym],
            out_specs=vmem,
            scratch_shapes=[
                pltpu.VMEM((vocab_dev, width), BF16),
                pltpu.VMEM((out_dev, width), BF16),
                pltpu.VMEM((PIECES, NDEV, ROWS, attn_dev), BF16),
                pltpu.VMEM((PIECES, 8, 8, piece_rows), F32),
                pltpu.VMEM((PIECES, NZ, 8, piece_rows), F32),
                dma((2,)),
                dma((NDEV,)),
                dma((NDEV,)),
                dma((PIECES, 12)),
                dma((PIECES, 12)),
            ] + exchange,
            compiler_params=pltpu.CompilerParams(collective_id=1, has_side_effects=True, vmem_limit_bytes=KERNEL_VMEM),
            cost_estimate=pl.CostEstimate(flops=40_000_000_000, bytes_accessed=8_000_000, transcendentals=0),
            name="back",
        )(attn_send, mlp, x_own, final_gain.reshape(1, width), next_rows, w_out_loc, embed_loc)
        log_probs = log_probs.reshape(steps, HALVES, NDEV, ROWS).transpose(0, 2, 1, 3).reshape(steps, batch)
        return log_probs, k_out, v_out

    cache_spec = P('tp', None, None)
    return jax.shard_map(device_fn, mesh=mesh, in_specs=(P(), P(), P(), P('tp', None), P(), P(None, 'tp'), P('tp', None), P(), cache_spec, cache_spec), out_specs=(P(), cache_spec, cache_spec), check_vma=False)
```

```python
import functools

import jax
import jax.numpy as jnp
from jax import lax
from jax.experimental import pallas as pl
from jax.experimental.pallas import tpu as pltpu
from jax.sharding import PartitionSpec as P

ROPE_BASE = 10000.0
NORM_EPS = 1e-6
MESH_ID = pl.DeviceIdType.MESH
ROWS = 8
LANES = 128
NZ = 4
NDEV = 32
STEPS = 2
HALVES = 2
PIECES = STEPS * HALVES
FRONT_ORDER = (
    "r00", "r10", "r01", "r11", "r20", "r30", "r02", "r12", "r21", "r03",
    "r13", "r31", "r04", "r22", "g00", "r14", "g10", "r32", "r23", "g01",
    "r33", "g11", "r24", "g20", "g12", "g02", "r34", "g30", "g21", "g03",
    "g31", "g13", "g22", "g32", "g04", "g14", "g23", "g24", "g33", "g34",
)
BACK_ORDER = (
    "r00", "r01", "r10", "r11", "r20", "r30", "r02", "r12", "r21", "r31",
    "r03", "r13", "r04", "g00", "r32", "r14", "g10", "r22", "r33", "g01",
    "g11", "r23", "g02", "r34", "g30", "r24", "g20", "g12", "g03", "g31",
    "g21", "g13", "g32", "g04", "g22", "g33", "g14", "g23", "g34", "g24",
)
KERNEL_VMEM = 60 * 1024 * 1024
BF16 = jnp.bfloat16
F32 = jnp.float32


def norm_rows(values, gain):
    centered = values - jnp.mean(values, axis=-1, keepdims=True)
    variance = jnp.mean(jnp.square(centered), axis=-1, keepdims=True)
    return (centered * lax.rsqrt(variance + NORM_EPS) * gain).astype(BF16)


def dot_nt(a, b):
    return lax.dot_general(a, b, (((1,), (1,)), ((), ())), preferred_element_type=F32)


class Place:
    def __init__(self):
        self.me = lax.axis_index("tp")
        self.c = lax.rem(self.me, 2)
        self.x = lax.rem(lax.div(self.me, 2), 2)
        self.y = lax.rem(lax.div(self.me, 4), 2)
        self.z = lax.div(self.me, 8)
        self.sib = self.me + 1 - 2 * self.c
        self.xpeer = self.me + 2 * (1 - 2 * self.x)
        self.ypeer = self.me + 4 * (1 - 2 * self.y)

    def zpeer(self, k):
        return lax.rem(self.me + 8 * k, NDEV)

    def peer(self, k):
        return lax.rem(self.me + k, NDEV)


def remote(src, dst, ssem, rsem, dev):
    return pltpu.make_async_remote_copy(src_ref=src, dst_ref=dst, send_sem=ssem, recv_sem=rsem, device_id=(dev,), device_id_type=MESH_ID)


def greet(place):
    barrier = pltpu.get_barrier_semaphore()

    def body(k, _):
        pl.semaphore_signal(barrier, inc=1, device_id=(place.peer(k),), device_id_type=MESH_ID)
        return 0

    lax.fori_loop(1, NDEV, body, 0)
    return barrier


def exchange_scratch(width):
    half = width // 2
    return dict(
        part=pltpu.VMEM((PIECES, NZ, 2, 2, 2, ROWS, width), BF16),
        rc=pltpu.VMEM((PIECES, NZ, 2, 2, ROWS, width), BF16),
        s1=pltpu.VMEM((PIECES, NZ, 2, 2, ROWS, width), BF16),
        r1a=pltpu.VMEM((PIECES, NZ, 2, ROWS, half), BF16),
        r1b=pltpu.VMEM((PIECES, NZ, 2, ROWS, half), BF16),
        s2a=pltpu.VMEM((PIECES, NZ, 2, ROWS, half), BF16),
        s2b=pltpu.VMEM((PIECES, NZ, 2, ROWS, half), BF16),
        r2a=pltpu.VMEM((PIECES, NZ, ROWS, half), BF16),
        r2b=pltpu.VMEM((PIECES, NZ, ROWS, half), BF16),
        s3=pltpu.VMEM((PIECES, NZ, ROWS, width), BF16),
        r3=pltpu.VMEM((PIECES, NZ - 1, ROWS, width), BF16),
        full=pltpu.VMEM((PIECES, NZ, 2, 2, 2, ROWS, width), BF16),
        rows=pltpu.VMEM((NDEV * ROWS, width), BF16),
        rs_s=pltpu.SemaphoreType.DMA((PIECES, 8)),
        rs_r=pltpu.SemaphoreType.DMA((PIECES, 8)),
        ag_s=pltpu.SemaphoreType.DMA((PIECES, 8)),
        ag_r=pltpu.SemaphoreType.DMA((PIECES, 8)),
    )


EXCHANGE_NAMES = ("part", "rc", "s1", "r1a", "r1b", "s2a", "s2b", "r2a", "r2b", "s3", "r3", "full", "rows", "rs_s", "rs_r", "ag_s", "ag_r")


def run_exchange(place, b, width, order, produce, barrier_wait, finalize, consume):
    x, y, z, c = place.x, place.y, place.z, place.c
    half = width // 2
    ca, cb = pl.ds(0, half), pl.ds(half, half)
    full = b["full"]
    sent = []

    def add(dst, left, right):
        dst[...] = (left[...].astype(F32) + right[...].astype(F32)).astype(BF16)

    def add_z(dst, left, right):
        def body(i, _):
            add(dst(i), left(i), right(i))
            return 0

        lax.fori_loop(0, NZ, body, 0)

    def rs_stages(n):
        live = {}

        def go(j, src, dst, dev):
            cp = remote(src, dst, b["rs_s"].at[n, j], b["rs_r"].at[n, j], dev)
            cp.start()
            live[j] = cp
            sent.append(cp)

        def st0():
            produce(n)
            barrier_wait()
            go(0, b["part"].at[n, :, :, :, 1 - c], b["rc"].at[n], place.sib)

        def st1():
            live[0].wait_recv()
            add_z(lambda i: b["s1"].at[n, i], lambda i: b["part"].at[n, i, :, :, c], lambda i: b["rc"].at[n, i])
            go(1, b["s1"].at[n, :, :, 1 - x, :, ca], b["r1a"].at[n], place.xpeer)
            go(2, b["s1"].at[n, :, 1 - y, :, :, cb], b["r1b"].at[n], place.ypeer)

        def st2():
            live[1].wait_recv()
            add_z(lambda i: b["s2a"].at[n, i], lambda i: b["s1"].at[n, i, :, x, :, ca], lambda i: b["r1a"].at[n, i])
            go(3, b["s2a"].at[n, :, 1 - y], b["r2a"].at[n], place.ypeer)
            live[2].wait_recv()
            add_z(lambda i: b["s2b"].at[n, i], lambda i: b["s1"].at[n, i, y, :, :, cb], lambda i: b["r1b"].at[n, i])
            go(4, b["s2b"].at[n, :, 1 - x], b["r2b"].at[n], place.xpeer)

        def st3():
            live[3].wait_recv()
            add(b["s3"].at[n, :, :, ca], b["s2a"].at[n, :, y], b["r2a"].at[n])
            live[4].wait_recv()
            add(b["s3"].at[n, :, :, cb], b["s2b"].at[n, :, x], b["r2b"].at[n])
            for k in range(1, NZ):
                go(4 + k, b["s3"].at[n, lax.rem(z + k, NZ)], b["r3"].at[n, k - 1], place.zpeer(k))

        def st4():
            for k in range(1, NZ):
                live[4 + k].wait_recv()

        return [st0, st1, st2, st3, st4]

    def ag_stages(n):
        live = {}

        def go(j, ref, dev):
            cp = remote(ref, ref, b["ag_s"].at[n, j], b["ag_r"].at[n, j], dev)
            cp.start()
            live[j] = cp
            sent.append(cp)

        def st0():
            total = b["s3"][n, z].astype(F32)
            for k in range(1, NZ):
                total = total + b["r3"][n, k - 1].astype(F32)
            full[n, z, y, x, c] = finalize(n, total)
            for k in range(1, NZ):
                go(k - 1, full.at[n, z, y, x, c], place.zpeer(k))

        def st1():
            for k in range(1, NZ):
                live[k - 1].wait_recv()
            go(3, full.at[n, :, y, x, c, :, ca], place.ypeer)
            go(4, full.at[n, :, y, x, c, :, cb], place.xpeer)

        def st2():
            live[3].wait_recv()
            go(5, full.at[n, :, :, x, c, :, ca], place.xpeer)
            live[4].wait_recv()
            go(6, full.at[n, :, y, :, c, :, cb], place.ypeer)

        def st3():
            live[5].wait_recv()
            live[6].wait_recv()
            go(7, full.at[n, :, :, :, c], place.sib)

        def st4():
            live[7].wait_recv()

            def body(i, _):
                block = full[n, i].astype(F32).reshape(8 * ROWS, width).astype(BF16)
                b["rows"][pl.ds(pl.multiple_of(i * 8 * ROWS, 8 * ROWS), 8 * ROWS), :] = block
                return 0

            lax.fori_loop(0, NZ, body, 0)
            consume(n)

        return [st0, st1, st2, st3, st4]

    stages = {"r": [rs_stages(n) for n in range(PIECES)], "g": [ag_stages(n) for n in range(PIECES)]}
    for item in order:
        with jax.named_scope(item):
            stages[item[0]][int(item[1])][int(item[2])]()
    for cp in sent:
        cp.wait_send()


def front_kernel(vocab_dev, width, qkv_dev, ff_dev, tok_ref, gain_ref, embed_ref, w_ref, x_ref, qkv_ref, mlp_ref,
                 emb, ids, hot, wq, wg, wu, sq, rq, local_sem, a_s, a_r, *bufs):
    b = dict(zip(EXCHANGE_NAMES, bufs))
    place = Place()
    me = place.me
    barrier = greet(place)
    batch = NDEV * HALVES * ROWS
    total = NDEV * ROWS
    tile = 512
    loads = []
    for h in range(width // tile):
        cols = pl.ds(h * tile, tile)
        loads.append(pltpu.make_async_copy(embed_ref.at[:, cols], emb.at[:, cols], local_sem.at[h]))
    pieces = ((wq.at[pl.ds(0, qkv_dev), :], 0, qkv_dev), (wg, qkv_dev, ff_dev), (wu, qkv_dev + ff_dev, ff_dev))
    for i, (dst, start, size) in enumerate(pieces):
        loads.append(pltpu.make_async_copy(w_ref.at[pl.ds(start, size), :], dst, local_sem.at[width // tile + i]))
    for cp in loads:
        cp.start()
    wq[qkv_dev:, :] = jnp.zeros((LANES - qkv_dev, width), BF16)
    vocab_start = me * vocab_dev
    for s in range(STEPS):
        row = jnp.broadcast_to((tok_ref[s:s + 1, :] - vocab_start).astype(F32), (8, batch))
        ids[s] = row.T.astype(jnp.int32).reshape(NDEV, HALVES, ROWS, 8)

    def produce(n):
        col = ids[n // HALVES, :, n % HALVES].reshape(total, 8)
        for i in range(2):
            lanes = lax.broadcasted_iota(jnp.int32, (total // 2, vocab_dev), 1)
            mine = col[i * total // 2:(i + 1) * total // 2, 0:1]
            hot[pl.ds(i * total // 2, total // 2), :] = jnp.where(mine == lanes, 1.0, 0.0).astype(BF16)
        for h in range(width // tile):
            cols = pl.ds(h * tile, tile)
            if n == 0:
                loads[h].wait()
            out = jnp.dot(hot[...], emb[:, cols], preferred_element_type=F32)
            b["part"][n, :, :, :, :, :, cols] = out.reshape(NZ, 2, 2, 2, ROWS, tile).astype(BF16)

    pending = [True]

    def barrier_wait():
        if pending[0]:
            pl.semaphore_wait(barrier, NDEV - 1)
            pending[0] = False

    def finalize(n, rows):
        x_ref[n] = rows.astype(BF16)
        return norm_rows(rows, gain_ref[...].astype(F32).reshape(1, width))

    def send_qkv(s, k):
        to = place.peer(k)
        pair = pl.ds(HALVES * s, HALVES)
        return remote(sq.at[pair, to], rq.at[me, pair], a_s.at[s, k], a_r.at[s, k], to)

    def consume(n):
        if n == 0:
            for cp in loads[width // tile:]:
                cp.wait()
        qkv = dot_nt(b["rows"][...], wq[...])
        sq[n] = qkv.reshape(NDEV, ROWS, LANES).astype(BF16)
        rq[me, n] = sq[n, me]
        if n % HALVES == HALVES - 1:
            def send(k, _):
                send_qkv(n // HALVES, k).start()
                return 0

            lax.fori_loop(1, NDEV, send, 0)
        gate = dot_nt(b["rows"][...], wg[...]).astype(BF16).astype(F32)
        up = dot_nt(b["rows"][...], wu[...]).astype(BF16).astype(F32)
        mlp_ref[n] = ((gate * (1.0 / (1.0 + jnp.exp(-gate)))) * up).astype(BF16)

    run_exchange(place, b, width, FRONT_ORDER, produce, barrier_wait, finalize, consume)
    with jax.named_scope("qkv_arrive"):
        for s in range(STEPS):
            def finish(k, _):
                cp = send_qkv(s, k)
                cp.wait_send()
                cp.wait_recv()
                return 0

            lax.fori_loop(1, NDEV, finish, 0)

    with jax.named_scope("qkv_out"):
        def copy_out(i, _):
            qkv_ref[i] = rq[i]
            return 0

        lax.fori_loop(0, NDEV, copy_out, 0)


def back_kernel(vocab_dev, width, attn_dev, ff_dev, scale, send_ref, mlp_ref, x_ref, gain_ref, next_ref, w_ref, embed_ref, out_ref,
                emb, wa, wv, ac, r8, r4, local_sem, a_s, a_r, st_s, st_r, *bufs):
    b = dict(zip(EXCHANGE_NAMES, bufs))
    place = Place()
    me = place.me
    r8[...] = jnp.zeros_like(r8)
    r4[...] = jnp.zeros_like(r4)
    barrier = greet(place)
    load_w = []
    for i, (start, size, dst) in enumerate(((0, attn_dev, wa.at[pl.ds(0, attn_dev), :]), (0, attn_dev, wa.at[pl.ds(attn_dev, attn_dev), :]), (attn_dev, ff_dev, wv))):
        load_w.append(pltpu.make_async_copy(w_ref.at[pl.ds(start, size), :], dst, local_sem.at[i]))
        load_w[-1].start()
    load_e = pltpu.make_async_copy(embed_ref, emb, local_sem.at[3])
    load_e.start()
    vocab_start = me * vocab_dev
    total = NDEV * ROWS

    def send_attn(k):
        to = place.peer(k)
        return remote(send_ref.at[to], ac.at[me], a_s.at[k], a_r.at[k], to)

    ac[me] = send_ref[me]
    with jax.named_scope("barrier"):
        pl.semaphore_wait(barrier, NDEV - 1)

    def send(k, _):
        send_attn(k).start()
        return 0

    with jax.named_scope("attn_send"):
        lax.fori_loop(1, NDEV, send, 0)
        for cp in load_w:
            cp.wait()

    def arrive(k, _):
        send_attn(k).wait_recv()
        return 0

    with jax.named_scope("attn_arrive"):
        lax.fori_loop(1, NDEV, arrive, 0)

    def produce(n):
        tile = 512
        att = ac[:, n % HALVES * ROWS:(n % HALVES + 1) * ROWS, :].astype(F32).reshape(total, LANES).astype(BF16)
        own = lax.broadcasted_iota(jnp.int32, (total, LANES), 1) // attn_dev == n // HALVES
        att = jnp.where(own, att, jnp.zeros_like(att))

        def mul(i, _):
            cols = pl.ds(pl.multiple_of(i * tile, tile), tile)
            out = jnp.dot(att, wa[:, cols], preferred_element_type=F32)
            out = out + jnp.dot(mlp_ref[n], wv[:, cols], preferred_element_type=F32)
            b["part"][n, :, :, :, :, :, cols] = out.reshape(NZ, 2, 2, 2, ROWS, tile).astype(BF16)
            return 0

        lax.fori_loop(0, width // tile, mul, 0)

    def finalize(n, rows):
        resid = x_ref[n].astype(F32) + rows.astype(BF16).astype(F32)
        return norm_rows(resid, gain_ref[...].astype(F32).reshape(1, width))

    plane = lax.rem(me, 8)

    def send_plane(n, k):
        q = lax.rem(plane + k, 8)
        return remote(r8.at[n, plane], r8.at[n, plane], st_s.at[n, k], st_r.at[n, k], me - plane + q)

    def send_line(n, k):
        return remote(r4.at[n, place.z], r4.at[n, place.z], st_s.at[n, 8 + k], st_r.at[n, 8 + k], place.zpeer(k))

    def consume(n):
        if n == 0:
            load_e.wait()
        tile = 512
        nxt = next_ref[n:n + 1, :] - vocab_start

        def mul(i, carry):
            top, den, hit = carry
            rows = pl.ds(pl.multiple_of(i * tile, tile), tile)
            logits = dot_nt(emb[rows, :], b["rows"][...]) * scale
            new = jnp.maximum(top, jnp.max(logits, axis=0, keepdims=True))
            den = den * jnp.exp(top - new) + jnp.sum(jnp.exp(logits - new), axis=0, keepdims=True)
            ids = lax.broadcasted_iota(jnp.int32, (tile, total), 0) + i * tile
            hit = hit + jnp.sum(jnp.where(ids == nxt, logits, 0.0), axis=0, keepdims=True)
            return new, den, hit

        zero = jnp.zeros((1, total), F32)
        top, den, hit = lax.fori_loop(0, vocab_dev // tile, mul, (jnp.full((1, total), -jnp.inf, F32), zero, zero))
        r8[n, plane, 0:1, :] = top
        r8[n, plane, 1:2, :] = den
        r8[n, plane, 2:3, :] = hit
        for k in range(1, 8):
            send_plane(n, k).start()

    def merge(buf, n, count):
        top = buf[n, 0, 0:1, :]
        for i in range(1, count):
            top = jnp.maximum(top, buf[n, i, 0:1, :])
        den = jnp.zeros_like(top)
        hit = jnp.zeros_like(top)
        for i in range(count):
            den = den + buf[n, i, 1:2, :] * jnp.exp(buf[n, i, 0:1, :] - top)
            hit = hit + buf[n, i, 2:3, :]
        return top, den, hit

    run_exchange(place, b, width, BACK_ORDER, produce, lambda: None, finalize, consume)
    last = [int(item[1]) for item in BACK_ORDER if item[0] == "g" and item[2] == "4"]
    for n in last:
        with jax.named_scope("plane"):
            for k in range(1, 8):
                send_plane(n, k).wait_recv()
            top, den, hit = merge(r8, n, 8)
            r4[n, place.z, 0:1, :] = top
            r4[n, place.z, 1:2, :] = den
            r4[n, place.z, 2:3, :] = hit
            for k in range(1, NZ):
                send_line(n, k).start()
    for n in last:
        with jax.named_scope("line"):
            for k in range(1, NZ):
                send_line(n, k).wait_recv()
            top, den, hit = merge(r4, n, NZ)
            out_ref[n:n + 1, :] = hit - top - jnp.log(den)
    for n in range(PIECES):
        for k in range(1, 8):
            send_plane(n, k).wait_send()
        for k in range(1, NZ):
            send_line(n, k).wait_send()

    def finish(k, _):
        send_attn(k).wait_send()
        return 0

    lax.fori_loop(1, NDEV, finish, 0)


def attention_kernel(heads, part_dev, lens_ref, qkv_ref, cos_ref, sin_ref, kc_ref, vc_ref, send_ref, ko_ref, vo_ref,
                     kbuf, vbuf, qry, knew, vnew, att, in_sem, out_sem):
    count, cache_len, head_dim = kc_ref.shape
    rows = STEPS * count
    ahead, group = 4, 2

    def load(i):
        return (pltpu.make_async_copy(kc_ref.at[i], kbuf.at[i], in_sem.at[0, i]),
                pltpu.make_async_copy(vc_ref.at[i], vbuf.at[i], in_sem.at[1, i]))

    def store(i):
        return (pltpu.make_async_copy(kbuf.at[i], ko_ref.at[i], out_sem.at[0, i]),
                pltpu.make_async_copy(vbuf.at[i], vo_ref.at[i], out_sem.at[1, i]))

    for i in range(ahead):
        for cp in load(i):
            cp.start()
    cosine, sine = cos_ref[...], sin_ref[...]
    parts = [qkv_ref[j].astype(F32).reshape(rows, LANES)[:, :part_dev] for j in range(NDEV)]
    for h in range(heads + 2):
        lo, hi = h * head_dim, (h + 1) * head_dim
        held = []
        for j in range(lo // part_dev, (hi - 1) // part_dev + 1):
            start, stop = max(lo, j * part_dev) - j * part_dev, min(hi, (j + 1) * part_dev) - j * part_dev
            held.append(parts[j][:, start:stop])
        vec = jnp.concatenate(held, axis=1)
        if h <= heads:
            vec = vec * cosine + pltpu.roll(vec, head_dim // 2, 1) * sine
        if h < heads:
            vec = vec * head_dim ** -0.5
            for s in range(STEPS):
                qry[pl.ds(s * heads + h, count, stride=STEPS * heads), :] = vec[s * count:(s + 1) * count]
        elif h == heads:
            knew[...] = vec
        else:
            vnew[...] = vec

    def one(i):
        first = lens_ref[i]
        for s in range(STEPS):
            pos = first + s
            base = pl.multiple_of(lax.div(pos, 16) * 16, 16)
            here = lax.broadcasted_iota(jnp.int32, (16, head_dim), 0) == pos - base
            for buf, new in ((kbuf, knew), (vbuf, vnew)):
                line = new[pl.ds(s * count + i, 1), :].astype(BF16)
                buf[i, pl.ds(base, 16), :] = jnp.where(here, line, buf[i, pl.ds(base, 16), :])
        query = qry[pl.ds(pl.multiple_of(i * STEPS * heads, STEPS * heads), STEPS * heads), :].astype(BF16)
        scores = dot_nt(query, kbuf[i])
        times = lax.broadcasted_iota(jnp.int32, scores.shape, 1)
        limit = first + jnp.where(lax.broadcasted_iota(jnp.int32, (STEPS * heads, 1), 0) >= heads, 1, 0)
        scores = jnp.where(times <= limit, scores, -jnp.inf)
        scores = jnp.exp(scores - jnp.max(scores, axis=1, keepdims=True))
        probs = (scores * (1.0 / jnp.sum(scores, axis=1, keepdims=True))).astype(BF16)
        out = jnp.dot(probs, vbuf[i], preferred_element_type=F32)
        old, new = out[:heads], out[heads:]
        low = lax.broadcasted_iota(jnp.int32, old.shape, 1) < head_dim // 2
        att[pl.ds(i, heads, stride=2 * count), :] = jnp.where(low, old, pltpu.roll(new, head_dim // 2, 1))
        att[pl.ds(count + i, heads, stride=2 * count), :] = jnp.where(low, pltpu.roll(old, head_dim // 2, 1), new)

    def body(g, _):
        for u in range(group):
            for cp in load(g * group + u):
                cp.wait()

        @pl.when(g < (count - ahead) // group)
        def _():
            for u in range(group):
                for cp in load(g * group + u + ahead):
                    cp.start()

        for u in range(group):
            one(g * group + u)
        for u in range(group):
            for cp in store(g * group + u):
                cp.start()
        return 0

    lax.fori_loop(0, count // group, body, 0)
    send_ref[...] = att[...].reshape(NDEV, count, LANES).astype(BF16)

    def drain(i, _):
        for cp in store(i):
            cp.wait()
        return 0

    lax.fori_loop(0, count, drain, 0)


def solution(mesh):
    def device_fn(tok_ids, next_ids, seq_lens, embed_loc, ln_gain, w_in_loc, w_out_loc, final_gain, k_loc, v_loc):
        steps, batch = tok_ids.shape
        vocab_dev, width = embed_loc.shape
        batch_dev, cache_len, head_dim = k_loc.shape
        in_dev, out_dev = w_in_loc.shape[1], w_out_loc.shape[0]
        kv_dev = 2 * head_dim // NDEV
        attn_dev = 2 * out_dev - in_dev + kv_dev
        ff_dev = out_dev - attn_dev
        qkv_dev = attn_dev + kv_dev
        attn_width = attn_dev * NDEV
        heads = attn_width // head_dim
        dev_index = lax.axis_index('tp')
        own_lens = lax.dynamic_slice_in_dim(seq_lens, dev_index * batch_dev, batch_dev)

        scratch = exchange_scratch(width)
        exchange = [scratch[name] for name in EXCHANGE_NAMES]
        vmem = pl.BlockSpec(memory_space=pltpu.VMEM)
        anym = pl.BlockSpec(memory_space=pltpu.HBM)
        dma = pltpu.SemaphoreType.DMA
        pair_dims = (steps, NDEV, HALVES, ROWS)
        piece_rows = NDEV * ROWS
        x_own, qkv_parts, mlp = pl.pallas_call(
            functools.partial(front_kernel, vocab_dev, width, qkv_dev, ff_dev),
            out_shape=(
                jax.ShapeDtypeStruct((PIECES, ROWS, width), BF16),
                jax.ShapeDtypeStruct((NDEV, PIECES, ROWS, LANES), BF16),
                jax.ShapeDtypeStruct((PIECES, piece_rows, ff_dev), BF16),
            ),
            in_specs=[vmem, vmem, anym, anym],
            out_specs=(vmem, vmem, vmem),
            scratch_shapes=[
                pltpu.VMEM((vocab_dev, width), BF16),
                pltpu.VMEM((steps, NDEV, HALVES, ROWS, 8), jnp.int32),
                pltpu.VMEM((piece_rows, vocab_dev), BF16),
                pltpu.VMEM((LANES, width), BF16),
                pltpu.VMEM((ff_dev, width), BF16),
                pltpu.VMEM((ff_dev, width), BF16),
                pltpu.VMEM((PIECES, NDEV, ROWS, LANES), BF16),
                pltpu.VMEM((NDEV, PIECES, ROWS, LANES), BF16),
                dma((8,)),
                dma((steps, NDEV)),
                dma((steps, NDEV)),
            ] + exchange,
            compiler_params=pltpu.CompilerParams(collective_id=0, has_side_effects=True, vmem_limit_bytes=KERNEL_VMEM),
            cost_estimate=pl.CostEstimate(flops=40_000_000_000, bytes_accessed=8_000_000, transcendentals=0),
            name="front",
        )(tok_ids, ln_gain, embed_loc, w_in_loc.T)

        half_dim = head_dim // 2
        inv_freq = ROPE_BASE ** (-jnp.arange(half_dim, dtype=jnp.float32) / half_dim)
        positions = own_lens[None, :] + jnp.arange(steps, dtype=own_lens.dtype)[:, None]
        angles = positions.reshape(-1, 1).astype(F32) * jnp.concatenate([inv_freq, inv_freq])
        sign = jnp.where(jnp.arange(head_dim) < half_dim, -1.0, 1.0)
        cosine, sine = jnp.cos(angles), jnp.sin(angles) * sign
        smem = pl.BlockSpec(memory_space=pltpu.SMEM)
        attn_send, k_out, v_out = pl.pallas_call(
            functools.partial(attention_kernel, heads, qkv_dev),
            out_shape=(
                jax.ShapeDtypeStruct((NDEV, batch_dev, LANES), BF16),
                jax.ShapeDtypeStruct(k_loc.shape, BF16),
                jax.ShapeDtypeStruct(v_loc.shape, BF16),
            ),
            in_specs=[smem, vmem, vmem, vmem, anym, anym],
            out_specs=(vmem, anym, anym),
            scratch_shapes=[
                pltpu.VMEM(k_loc.shape, BF16),
                pltpu.VMEM(v_loc.shape, BF16),
                pltpu.VMEM((batch_dev * steps * heads, head_dim), F32),
                pltpu.VMEM((steps * batch_dev, head_dim), F32),
                pltpu.VMEM((steps * batch_dev, head_dim), F32),
                pltpu.VMEM((NDEV * batch_dev, LANES), F32),
                dma((2, batch_dev)),
                dma((2, batch_dev)),
            ],
            compiler_params=pltpu.CompilerParams(vmem_limit_bytes=KERNEL_VMEM),
            cost_estimate=pl.CostEstimate(flops=1_000_000_000, bytes_accessed=34_000_000, transcendentals=0),
            name="attention",
        )(own_lens, qkv_parts, cosine, sine, k_loc, v_loc)

        next_rows = next_ids.reshape(pair_dims).transpose(0, 2, 1, 3).reshape(PIECES, piece_rows)
        log_probs = pl.pallas_call(
            functools.partial(back_kernel, vocab_dev, width, attn_dev, ff_dev, width ** -0.5),
            out_shape=jax.ShapeDtypeStruct((PIECES, piece_rows), F32),
            in_specs=[vmem, vmem, vmem, vmem, vmem, anym, anym],
            out_specs=vmem,
            scratch_shapes=[
                pltpu.VMEM((vocab_dev, width), BF16),
                pltpu.VMEM((2 * attn_dev, width), BF16),
                pltpu.VMEM((ff_dev, width), BF16),
                pltpu.VMEM((NDEV, batch_dev, LANES), BF16),
                pltpu.VMEM((PIECES, 8, 8, piece_rows), F32),
                pltpu.VMEM((PIECES, NZ, 8, piece_rows), F32),
                dma((4,)),
                dma((NDEV,)),
                dma((NDEV,)),
                dma((PIECES, 12)),
                dma((PIECES, 12)),
            ] + exchange,
            compiler_params=pltpu.CompilerParams(collective_id=1, has_side_effects=True, vmem_limit_bytes=KERNEL_VMEM),
            cost_estimate=pl.CostEstimate(flops=40_000_000_000, bytes_accessed=8_000_000, transcendentals=0),
            name="back",
        )(attn_send, mlp, x_own, final_gain, next_rows, w_out_loc, embed_loc)
        log_probs = log_probs.reshape(steps, HALVES, NDEV, ROWS).transpose(0, 2, 1, 3).reshape(steps, batch)
        return log_probs, k_out, v_out

    cache_spec = P('tp', None, None)
    return jax.shard_map(device_fn, mesh=mesh, in_specs=(P(), P(), P(), P('tp', None), P(), P(None, 'tp'), P('tp', None), P(), cache_spec, cache_spec), out_specs=(P(), cache_spec, cache_spec), check_vma=False)
```

```python
import functools

import jax
import jax.numpy as jnp
from jax import lax
from jax.experimental import pallas as pl
from jax.experimental.pallas import tpu as pltpu
from jax.sharding import PartitionSpec as P

ROPE_BASE = 10000.0
NORM_EPS = 1e-6
MESH_ID = pl.DeviceIdType.MESH
ROWS = 8
LANES = 128
NZ = 4
NDEV = 32
STEPS = 2
HALVES = 2
PIECES = STEPS * HALVES
SPLIT = 2
FRONT_ORDER = (
    "r000", "r010", "r001", "r100", "r011", "r110", "r101", "r200", "r002", "r111",
    "r012", "r210", "r300", "r102", "r003", "r310", "r112", "r201", "r013", "r211",
    "r103", "r301", "r311", "r113", "r014", "r004", "g000", "g010", "r212", "r202",
    "r302", "r114", "r104", "g100", "r312", "g001", "g110", "r213", "r203", "g101",
    "r313", "g011", "r303", "g111", "g102", "g012", "r214", "r204", "g200", "g002",
    "g210", "g112", "g013", "r304", "r314", "g300", "g310", "g201", "g211", "g003",
    "g113", "g202", "g114", "g004", "g301", "g311", "g103", "g014", "g212", "c000",
    "c001", "g302", "g312", "g203", "g104", "c100", "c101", "g204", "g303", "g213",
    "g313", "g304", "t000", "g214", "c200", "g314", "c300", "t100", "c201", "c301",
)
BACK_ORDER = (
    "r000", "r010", "r001", "r100", "r011", "r110", "r200", "r101", "r210", "r002",
    "r012", "r111", "r300", "r310", "r102", "r201", "r003", "r211", "r013", "r112",
    "r103", "r004", "r301", "r014", "g000", "r212", "g010", "r113", "r202", "g001",
    "r311", "r104", "r213", "g011", "r203", "g002", "r302", "r114", "g100", "g110",
    "g012", "r312", "r204", "r214", "g200", "g210", "g003", "g101", "g013", "g111",
    "r313", "g004", "r303", "g102", "g014", "c000", "g201", "g112", "g211", "c001",
    "c002", "g202", "g103", "r314", "r304", "g300", "g104", "g310", "g113", "g212",
    "t000", "g114", "g301", "c100", "g311", "c101", "g213", "g302", "g203", "c102",
    "g312", "g204", "g214", "c200", "c201", "t100", "g303", "g313", "c202", "g304",
    "g314", "c300", "c301", "c302", "t200", "t001", "t300", "t101", "t201", "t301",
)
FRONT_FIRST, BACK_FIRST = 0, 0
KERNEL_VMEM = 60 * 1024 * 1024
BF16 = jnp.bfloat16
F32 = jnp.float32


def norm_rows(values, gain):
    centered = values - jnp.mean(values, axis=-1, keepdims=True)
    variance = jnp.mean(jnp.square(centered), axis=-1, keepdims=True)
    return (centered * lax.rsqrt(variance + NORM_EPS) * gain).astype(BF16)


def dot_nt(a, b):
    return lax.dot_general(a, b, (((1,), (1,)), ((), ())), preferred_element_type=F32)


class Place:
    def __init__(self):
        self.me = lax.axis_index("tp")
        self.c = lax.rem(self.me, 2)
        self.x = lax.rem(lax.div(self.me, 2), 2)
        self.y = lax.rem(lax.div(self.me, 4), 2)
        self.z = lax.div(self.me, 8)
        self.sib = self.me + 1 - 2 * self.c
        self.xpeer = self.me + 2 * (1 - 2 * self.x)
        self.ypeer = self.me + 4 * (1 - 2 * self.y)

    def zpeer(self, k):
        return lax.rem(self.me + 8 * k, NDEV)

    def peer(self, k):
        return lax.rem(self.me + k, NDEV)


def remote(src, dst, ssem, rsem, dev):
    return pltpu.make_async_remote_copy(src_ref=src, dst_ref=dst, send_sem=ssem, recv_sem=rsem, device_id=(dev,), device_id_type=MESH_ID)


def greet(place):
    barrier = pltpu.get_barrier_semaphore()

    def body(k, _):
        pl.semaphore_signal(barrier, inc=1, device_id=(place.peer(k),), device_id_type=MESH_ID)
        return 0

    lax.fori_loop(1, NDEV, body, 0)
    return barrier


def exchange_scratch(width):
    part = width // SPLIT
    lead = (PIECES, SPLIT)
    return dict(
        part=pltpu.VMEM((PIECES, NZ, 2, 2, 2, ROWS, width), BF16),
        rc=pltpu.VMEM((PIECES, NZ, 2, 2, ROWS, width), BF16),
        s1=pltpu.VMEM((PIECES, NZ, 2, 2, ROWS, width), BF16),
        r1a=pltpu.VMEM(lead + (NZ, 2, ROWS, part // 2), BF16),
        r1b=pltpu.VMEM(lead + (NZ, 2, ROWS, part // 2), BF16),
        s2a=pltpu.VMEM(lead + (NZ, 2, ROWS, part // 2), BF16),
        s2b=pltpu.VMEM(lead + (NZ, 2, ROWS, part // 2), BF16),
        r2a=pltpu.VMEM(lead + (NZ, ROWS, part // 2), BF16),
        r2b=pltpu.VMEM(lead + (NZ, ROWS, part // 2), BF16),
        s3=pltpu.VMEM((PIECES, NZ, ROWS, width), BF16),
        r3=pltpu.VMEM((PIECES, NZ - 1, ROWS, width), BF16),
        full=pltpu.VMEM((PIECES, NZ, 2, 2, 2, ROWS, width), BF16),
        rows=pltpu.VMEM((PIECES, NDEV * ROWS, width), BF16),
        rs_s=pltpu.SemaphoreType.DMA((PIECES, SPLIT * 8)),
        rs_r=pltpu.SemaphoreType.DMA((PIECES, SPLIT * 8)),
        ag_s=pltpu.SemaphoreType.DMA((PIECES, SPLIT * 8)),
        ag_r=pltpu.SemaphoreType.DMA((PIECES, SPLIT * 8)),
    )


EXCHANGE_NAMES = ("part", "rc", "s1", "r1a", "r1b", "s2a", "s2b", "r2a", "r2b", "s3", "r3", "full", "rows", "rs_s", "rs_r", "ag_s", "ag_r")


def run_exchange(place, b, width, order, produce, barrier_wait, finalize, consume, after):
    x, y, z, c = place.x, place.y, place.z, place.c
    wide = width // SPLIT
    half = wide // 2
    full = b["full"]
    sent = []

    def add(dst, left, right):
        dst[...] = (left[...].astype(F32) + right[...].astype(F32)).astype(BF16)

    def add_z(dst, left, right):
        def body(i, _):
            add(dst(i), left(i), right(i))
            return 0

        lax.fori_loop(0, NZ, body, 0)

    def rs_stages(n, h):
        live = {}
        cols = pl.ds(h * wide, wide)
        ca, cb = pl.ds(h * wide, half), pl.ds(h * wide + half, half)

        def go(j, src, dst, dev):
            cp = remote(src, dst, b["rs_s"].at[n, h * 8 + j], b["rs_r"].at[n, h * 8 + j], dev)
            cp.start()
            live[j] = cp
            sent.append(cp)

        def st0():
            produce(n, h)
            barrier_wait()
            go(0, b["part"].at[n, :, :, :, 1 - c, :, cols], b["rc"].at[n, :, :, :, :, cols], place.sib)

        def st1():
            live[0].wait_recv()
            add_z(lambda i: b["s1"].at[n, i, :, :, :, cols], lambda i: b["part"].at[n, i, :, :, c, :, cols], lambda i: b["rc"].at[n, i, :, :, :, cols])
            go(1, b["s1"].at[n, :, :, 1 - x, :, ca], b["r1a"].at[n, h], place.xpeer)
            go(2, b["s1"].at[n, :, 1 - y, :, :, cb], b["r1b"].at[n, h], place.ypeer)

        def st2():
            live[1].wait_recv()
            add_z(lambda i: b["s2a"].at[n, h, i], lambda i: b["s1"].at[n, i, :, x, :, ca], lambda i: b["r1a"].at[n, h, i])
            go(3, b["s2a"].at[n, h, :, 1 - y], b["r2a"].at[n, h], place.ypeer)
            live[2].wait_recv()
            add_z(lambda i: b["s2b"].at[n, h, i], lambda i: b["s1"].at[n, i, y, :, :, cb], lambda i: b["r1b"].at[n, h, i])
            go(4, b["s2b"].at[n, h, :, 1 - x], b["r2b"].at[n, h], place.xpeer)

        def st3():
            live[3].wait_recv()
            add(b["s3"].at[n, :, :, ca], b["s2a"].at[n, h, :, y], b["r2a"].at[n, h])
            live[4].wait_recv()
            add(b["s3"].at[n, :, :, cb], b["s2b"].at[n, h, :, x], b["r2b"].at[n, h])
            for k in range(1, NZ):
                go(4 + k, b["s3"].at[n, lax.rem(z + k, NZ), :, cols], b["r3"].at[n, k - 1, :, cols], place.zpeer(k))

        def st4():
            for k in range(1, NZ):
                live[4 + k].wait_recv()

        return [st0, st1, st2, st3, st4]

    def ag_stages(n, h):
        live = {}
        cols = pl.ds(h * wide, wide)
        ca, cb = pl.ds(h * wide, half), pl.ds(h * wide + half, half)

        def go(j, ref, dev):
            cp = remote(ref, ref, b["ag_s"].at[n, h * 8 + j], b["ag_r"].at[n, h * 8 + j], dev)
            cp.start()
            live[j] = cp
            sent.append(cp)

        def st0():
            if h == 0:
                total = b["s3"][n, z].astype(F32)
                for k in range(1, NZ):
                    total = total + b["r3"][n, k - 1].astype(F32)
                full[n, z, y, x, c] = finalize(n, total)
            for k in range(1, NZ):
                go(k - 1, full.at[n, z, y, x, c, :, cols], place.zpeer(k))

        def st1():
            for k in range(1, NZ):
                live[k - 1].wait_recv()
            go(3, full.at[n, :, y, x, c, :, ca], place.ypeer)
            go(4, full.at[n, :, y, x, c, :, cb], place.xpeer)

        def st2():
            live[3].wait_recv()
            go(5, full.at[n, :, :, x, c, :, ca], place.xpeer)
            live[4].wait_recv()
            go(6, full.at[n, :, y, :, c, :, cb], place.ypeer)

        def st3():
            live[5].wait_recv()
            live[6].wait_recv()
            go(7, full.at[n, :, :, :, c, :, cols], place.sib)

        def st4():
            live[7].wait_recv()

            def body(i, _):
                block = full[n, i, :, :, :, :, cols].astype(F32).reshape(8 * ROWS, wide).astype(BF16)
                b["rows"][n, pl.ds(pl.multiple_of(i * 8 * ROWS, 8 * ROWS), 8 * ROWS), cols] = block
                return 0

            lax.fori_loop(0, NZ, body, 0)

        return [st0, st1, st2, st3, st4]

    scatter = [[rs_stages(n, h) for h in range(SPLIT)] for n in range(PIECES)]
    gather = [[ag_stages(n, h) for h in range(SPLIT)] for n in range(PIECES)]
    for item in order:
        kind, n, h, j = item[0], int(item[1]), int(item[2]), int(item[3])
        with jax.named_scope(item):
            if kind == "r":
                scatter[n][h][j]()
            elif kind == "g":
                gather[n][h][j]()
            elif kind == "c":
                consume(n, j)
            else:
                after(n, j)
    for cp in sent:
        cp.wait_send()


def front_kernel(vocab_dev, width, qkv_dev, ff_dev, tok_ref, gain_ref, embed_ref, w_ref, x_ref, qkv_ref, mlp_ref,
                 emb, ids, hot, wq, wg, wu, sq, rq, local_sem, a_s, a_r, *bufs):
    b = dict(zip(EXCHANGE_NAMES, bufs))
    place = Place()
    me = place.me
    barrier = greet(place)
    batch = NDEV * HALVES * ROWS
    total = NDEV * ROWS
    tile = 512
    loads = []
    for h in range(width // tile):
        cols = pl.ds(h * tile, tile)
        loads.append(pltpu.make_async_copy(embed_ref.at[:, cols], emb.at[:, cols], local_sem.at[h]))
    pieces = ((wq.at[pl.ds(0, qkv_dev), :], 0, qkv_dev), (wg, qkv_dev, ff_dev), (wu, qkv_dev + ff_dev, ff_dev))
    for i, (dst, start, size) in enumerate(pieces):
        loads.append(pltpu.make_async_copy(w_ref.at[pl.ds(start, size), :], dst, local_sem.at[width // tile + i]))
    for cp in loads:
        cp.start()
    wq[qkv_dev:, :] = jnp.zeros((LANES - qkv_dev, width), BF16)
    vocab_start = me * vocab_dev
    for s in range(STEPS):
        row = jnp.broadcast_to((tok_ref[s:s + 1, :] - vocab_start).astype(F32), (8, batch))
        ids[s] = row.T.astype(jnp.int32).reshape(NDEV, HALVES, ROWS, 8)

    def produce(n, part):
        if part == 0:
            build(n)
        for h in range(part * width // SPLIT // tile, (part + 1) * width // SPLIT // tile):
            cols = pl.ds(h * tile, tile)
            if n == 0:
                loads[h].wait()
            out = jnp.dot(hot[...], emb[:, cols], preferred_element_type=F32)
            b["part"][n, :, :, :, :, :, cols] = out.reshape(NZ, 2, 2, 2, ROWS, tile).astype(BF16)

    def build(n):
        col = ids[n // HALVES, :, n % HALVES].reshape(total, 8)
        for i in range(2):
            lanes = lax.broadcasted_iota(jnp.int32, (total // 2, vocab_dev), 1)
            mine = col[i * total // 2:(i + 1) * total // 2, 0:1]
            hot[pl.ds(i * total // 2, total // 2), :] = jnp.where(mine == lanes, 1.0, 0.0).astype(BF16)

    pending = [True]

    def barrier_wait():
        if pending[0]:
            pl.semaphore_wait(barrier, NDEV - 1)
            pending[0] = False

    def finalize(n, rows):
        x_ref[n] = rows.astype(BF16)
        return norm_rows(rows, gain_ref[...].astype(F32).reshape(1, width))

    def send_qkv(s, k):
        to = place.peer(k)
        pair = pl.ds(HALVES * s, HALVES)
        return remote(sq.at[pair, to], rq.at[me, pair], a_s.at[s, k], a_r.at[s, k], to)

    def consume(n, j):
        if n == FRONT_FIRST and j == 0:
            for cp in loads[width // tile:]:
                cp.wait()
        hid = b["rows"].at[n]
        if j == 0:
            qkv = dot_nt(hid[...], wq[...])
            sq[n] = qkv.reshape(NDEV, ROWS, LANES).astype(BF16)
            rq[me, n] = sq[n, me]
        else:
            gate = dot_nt(hid[...], wg[...]).astype(BF16).astype(F32)
            up = dot_nt(hid[...], wu[...]).astype(BF16).astype(F32)
            mlp_ref[n] = ((gate * (1.0 / (1.0 + jnp.exp(-gate)))) * up).astype(BF16)

    def after(s, _):
        def send(k, _):
            send_qkv(s, k).start()
            return 0

        lax.fori_loop(1, NDEV, send, 0)

    run_exchange(place, b, width, FRONT_ORDER, produce, barrier_wait, finalize, consume, after)
    with jax.named_scope("qkv_arrive"):
        for s in range(STEPS):
            def finish(k, _):
                cp = send_qkv(s, k)
                cp.wait_send()
                cp.wait_recv()
                return 0

            lax.fori_loop(1, NDEV, finish, 0)

    with jax.named_scope("qkv_out"):
        def copy_out(i, _):
            qkv_ref[i] = rq[i]
            return 0

        lax.fori_loop(0, NDEV, copy_out, 0)


def back_kernel(vocab_dev, width, attn_dev, ff_dev, scale, send_ref, mlp_ref, x_ref, gain_ref, next_ref, w_ref, embed_ref, out_ref,
                emb, wa, wv, ac, run, r8, r4, local_sem, a_s, a_r, st_s, st_r, *bufs):
    b = dict(zip(EXCHANGE_NAMES, bufs))
    place = Place()
    me = place.me
    r8[...] = jnp.zeros_like(r8)
    r4[...] = jnp.zeros_like(r4)
    barrier = greet(place)
    load_w = []
    for i, (start, size, dst) in enumerate(((0, attn_dev, wa.at[pl.ds(0, attn_dev), :]), (0, attn_dev, wa.at[pl.ds(attn_dev, attn_dev), :]), (attn_dev, ff_dev, wv))):
        load_w.append(pltpu.make_async_copy(w_ref.at[pl.ds(start, size), :], dst, local_sem.at[i]))
        load_w[-1].start()
    load_e = pltpu.make_async_copy(embed_ref, emb, local_sem.at[3])
    load_e.start()
    vocab_start = me * vocab_dev
    total = NDEV * ROWS

    def send_attn(k):
        to = place.peer(k)
        return remote(send_ref.at[to], ac.at[me], a_s.at[k], a_r.at[k], to)

    ac[me] = send_ref[me]
    with jax.named_scope("barrier"):
        pl.semaphore_wait(barrier, NDEV - 1)

    def send(k, _):
        send_attn(k).start()
        return 0

    with jax.named_scope("attn_send"):
        lax.fori_loop(1, NDEV, send, 0)
        for cp in load_w:
            cp.wait()

    def arrive(k, _):
        send_attn(k).wait_recv()
        return 0

    with jax.named_scope("attn_arrive"):
        lax.fori_loop(1, NDEV, arrive, 0)

    def produce(n, part):
        tile = 512
        per = width // SPLIT // tile
        att = ac[:, n % HALVES * ROWS:(n % HALVES + 1) * ROWS, :].astype(F32).reshape(total, LANES).astype(BF16)
        own = lax.broadcasted_iota(jnp.int32, (total, LANES), 1) // attn_dev == n // HALVES
        att = jnp.where(own, att, jnp.zeros_like(att))

        def mul(i, _):
            cols = pl.ds(pl.multiple_of((part * per + i) * tile, tile), tile)
            out = jnp.dot(att, wa[:, cols], preferred_element_type=F32)
            out = out + jnp.dot(mlp_ref[n], wv[:, cols], preferred_element_type=F32)
            b["part"][n, :, :, :, :, :, cols] = out.reshape(NZ, 2, 2, 2, ROWS, tile).astype(BF16)
            return 0

        lax.fori_loop(0, per, mul, 0)

    def finalize(n, rows):
        resid = x_ref[n].astype(F32) + rows.astype(BF16).astype(F32)
        return norm_rows(resid, gain_ref[...].astype(F32).reshape(1, width))

    plane = lax.rem(me, 8)

    def send_plane(n, k):
        q = lax.rem(plane + k, 8)
        return remote(r8.at[n, plane], r8.at[n, plane], st_s.at[n, k], st_r.at[n, k], me - plane + q)

    def send_line(n, k):
        return remote(r4.at[n, place.z], r4.at[n, place.z], st_s.at[n, 8 + k], st_r.at[n, 8 + k], place.zpeer(k))

    def pack(ref, top, den, hit):
        for i, value in enumerate((top, den, hit)):
            ref[2 * i:2 * i + 1, :] = value[:, :LANES]
            ref[2 * i + 1:2 * i + 2, :] = value[:, LANES:]

    def consume(n, j):
        if n == BACK_FIRST and j == 0:
            load_e.wait()
        tile = vocab_dev // 3
        logits = dot_nt(emb[j * tile:(j + 1) * tile, :], b["rows"][n]) * scale
        nxt = next_ref[n:n + 1, :] - vocab_start
        ids = lax.broadcasted_iota(jnp.int32, (tile, total), 0) + j * tile
        top = jnp.max(logits, axis=0, keepdims=True)
        hit = jnp.sum(jnp.where(ids == nxt, logits, 0.0), axis=0, keepdims=True)
        if j > 0:
            was, den = run[n, 0:1, :], run[n, 1:2, :]
            top = jnp.maximum(was, top)
            hit = run[n, 2:3, :] + hit
        more = jnp.sum(jnp.exp(logits - top), axis=0, keepdims=True)
        den = den * jnp.exp(was - top) + more if j > 0 else more
        if j < 2:
            run[n, 0:1, :] = top
            run[n, 1:2, :] = den
            run[n, 2:3, :] = hit
            return
        pack(r8.at[n, plane], top, den, hit)
        for k in range(1, 8):
            send_plane(n, k).start()

    def merge(buf, n, count):
        top = buf[n, 0, 0:2, :]
        for i in range(1, count):
            top = jnp.maximum(top, buf[n, i, 0:2, :])
        den = jnp.zeros_like(top)
        hit = jnp.zeros_like(top)
        for i in range(count):
            den = den + buf[n, i, 2:4, :] * jnp.exp(buf[n, i, 0:2, :] - top)
            hit = hit + buf[n, i, 4:6, :]
        return top, den, hit

    def after(n, j):
        if j == 0:
            for k in range(1, 8):
                send_plane(n, k).wait_recv()
            top, den, hit = merge(r8, n, 8)
            r4[n, place.z, 0:2, :] = top
            r4[n, place.z, 2:4, :] = den
            r4[n, place.z, 4:6, :] = hit
            for k in range(1, NZ):
                send_line(n, k).start()
        else:
            for k in range(1, NZ):
                send_line(n, k).wait_recv()
            top, den, hit = merge(r4, n, NZ)
            out_ref[2 * n:2 * n + 2, :] = hit - top - jnp.log(den)

    run_exchange(place, b, width, BACK_ORDER, produce, lambda: None, finalize, consume, after)
    for n in range(PIECES):
        for k in range(1, 8):
            send_plane(n, k).wait_send()
        for k in range(1, NZ):
            send_line(n, k).wait_send()

    def finish(k, _):
        send_attn(k).wait_send()
        return 0

    lax.fori_loop(1, NDEV, finish, 0)


def attention_kernel(heads, part_dev, lens_ref, qkv_ref, cos_ref, sin_ref, kc_ref, vc_ref, send_ref, ko_ref, vo_ref,
                     kbuf, vbuf, qry, knew, vnew, att, in_sem, out_sem):
    count, cache_len, head_dim = kc_ref.shape
    rows = STEPS * count
    ahead, group = 4, 2

    def load(i):
        return (pltpu.make_async_copy(kc_ref.at[i], kbuf.at[i], in_sem.at[0, i]),
                pltpu.make_async_copy(vc_ref.at[i], vbuf.at[i], in_sem.at[1, i]))

    def store(i):
        return (pltpu.make_async_copy(kbuf.at[i], ko_ref.at[i], out_sem.at[0, i]),
                pltpu.make_async_copy(vbuf.at[i], vo_ref.at[i], out_sem.at[1, i]))

    for i in range(ahead):
        for cp in load(i):
            cp.start()
    cosine, sine = cos_ref[...], sin_ref[...]
    parts = [qkv_ref[j].astype(F32).reshape(rows, LANES)[:, :part_dev] for j in range(NDEV)]
    for h in range(heads + 2):
        lo, hi = h * head_dim, (h + 1) * head_dim
        held = []
        for j in range(lo // part_dev, (hi - 1) // part_dev + 1):
            start, stop = max(lo, j * part_dev) - j * part_dev, min(hi, (j + 1) * part_dev) - j * part_dev
            held.append(parts[j][:, start:stop])
        vec = jnp.concatenate(held, axis=1)
        if h <= heads:
            vec = vec * cosine + pltpu.roll(vec, head_dim // 2, 1) * sine
        if h < heads:
            vec = vec * head_dim ** -0.5
            for s in range(STEPS):
                qry[pl.ds(s * heads + h, count, stride=STEPS * heads), :] = vec[s * count:(s + 1) * count]
        elif h == heads:
            knew[...] = vec
        else:
            vnew[...] = vec

    def one(i):
        first = lens_ref[i]
        for s in range(STEPS):
            pos = first + s
            base = pl.multiple_of(lax.div(pos, 16) * 16, 16)
            here = lax.broadcasted_iota(jnp.int32, (16, head_dim), 0) == pos - base
            for buf, new in ((kbuf, knew), (vbuf, vnew)):
                line = new[pl.ds(s * count + i, 1), :].astype(BF16)
                buf[i, pl.ds(base, 16), :] = jnp.where(here, line, buf[i, pl.ds(base, 16), :])
        query = qry[pl.ds(pl.multiple_of(i * STEPS * heads, STEPS * heads), STEPS * heads), :].astype(BF16)
        scores = dot_nt(query, kbuf[i])
        times = lax.broadcasted_iota(jnp.int32, scores.shape, 1)
        limit = first + jnp.where(lax.broadcasted_iota(jnp.int32, (STEPS * heads, 1), 0) >= heads, 1, 0)
        scores = jnp.where(times <= limit, scores, -jnp.inf)
        scores = jnp.exp(scores - jnp.max(scores, axis=1, keepdims=True))
        probs = (scores * (1.0 / jnp.sum(scores, axis=1, keepdims=True))).astype(BF16)
        out = jnp.dot(probs, vbuf[i], preferred_element_type=F32)
        old, new = out[:heads], out[heads:]
        low = lax.broadcasted_iota(jnp.int32, old.shape, 1) < head_dim // 2
        att[pl.ds(i, heads, stride=2 * count), :] = jnp.where(low, old, pltpu.roll(new, head_dim // 2, 1))
        att[pl.ds(count + i, heads, stride=2 * count), :] = jnp.where(low, pltpu.roll(old, head_dim // 2, 1), new)

    def body(g, _):
        for u in range(group):
            for cp in load(g * group + u):
                cp.wait()

        @pl.when(g < (count - ahead) // group)
        def _():
            for u in range(group):
                for cp in load(g * group + u + ahead):
                    cp.start()

        for u in range(group):
            one(g * group + u)
        for u in range(group):
            for cp in store(g * group + u):
                cp.start()
        return 0

    lax.fori_loop(0, count // group, body, 0)
    send_ref[...] = att[...].reshape(NDEV, count, LANES).astype(BF16)

    def drain(i, _):
        for cp in store(i):
            cp.wait()
        return 0

    lax.fori_loop(0, count, drain, 0)


def solution(mesh):
    def device_fn(tok_ids, next_ids, seq_lens, embed_loc, ln_gain, w_in_loc, w_out_loc, final_gain, k_loc, v_loc):
        steps, batch = tok_ids.shape
        vocab_dev, width = embed_loc.shape
        batch_dev, cache_len, head_dim = k_loc.shape
        in_dev, out_dev = w_in_loc.shape[1], w_out_loc.shape[0]
        kv_dev = 2 * head_dim // NDEV
        attn_dev = 2 * out_dev - in_dev + kv_dev
        ff_dev = out_dev - attn_dev
        qkv_dev = attn_dev + kv_dev
        attn_width = attn_dev * NDEV
        heads = attn_width // head_dim
        dev_index = lax.axis_index('tp')
        own_lens = lax.dynamic_slice_in_dim(seq_lens, dev_index * batch_dev, batch_dev)

        scratch = exchange_scratch(width)
        exchange = [scratch[name] for name in EXCHANGE_NAMES]
        vmem = pl.BlockSpec(memory_space=pltpu.VMEM)
        anym = pl.BlockSpec(memory_space=pltpu.HBM)
        dma = pltpu.SemaphoreType.DMA
        pair_dims = (steps, NDEV, HALVES, ROWS)
        piece_rows = NDEV * ROWS
        x_own, qkv_parts, mlp = pl.pallas_call(
            functools.partial(front_kernel, vocab_dev, width, qkv_dev, ff_dev),
            out_shape=(
                jax.ShapeDtypeStruct((PIECES, ROWS, width), BF16),
                jax.ShapeDtypeStruct((NDEV, PIECES, ROWS, LANES), BF16),
                jax.ShapeDtypeStruct((PIECES, piece_rows, ff_dev), BF16),
            ),
            in_specs=[vmem, vmem, anym, anym],
            out_specs=(vmem, vmem, vmem),
            scratch_shapes=[
                pltpu.VMEM((vocab_dev, width), BF16),
                pltpu.VMEM((steps, NDEV, HALVES, ROWS, 8), jnp.int32),
                pltpu.VMEM((piece_rows, vocab_dev), BF16),
                pltpu.VMEM((LANES, width), BF16),
                pltpu.VMEM((ff_dev, width), BF16),
                pltpu.VMEM((ff_dev, width), BF16),
                pltpu.VMEM((PIECES, NDEV, ROWS, LANES), BF16),
                pltpu.VMEM((NDEV, PIECES, ROWS, LANES), BF16),
                dma((8,)),
                dma((steps, NDEV)),
                dma((steps, NDEV)),
            ] + exchange,
            compiler_params=pltpu.CompilerParams(collective_id=0, has_side_effects=True, vmem_limit_bytes=KERNEL_VMEM),
            cost_estimate=pl.CostEstimate(flops=40_000_000_000, bytes_accessed=8_000_000, transcendentals=0),
            name="front",
        )(tok_ids, ln_gain, embed_loc, w_in_loc.T)

        half_dim = head_dim // 2
        inv_freq = ROPE_BASE ** (-jnp.arange(half_dim, dtype=jnp.float32) / half_dim)
        positions = own_lens[None, :] + jnp.arange(steps, dtype=own_lens.dtype)[:, None]
        angles = positions.reshape(-1, 1).astype(F32) * jnp.concatenate([inv_freq, inv_freq])
        sign = jnp.where(jnp.arange(head_dim) < half_dim, -1.0, 1.0)
        cosine, sine = jnp.cos(angles), jnp.sin(angles) * sign
        smem = pl.BlockSpec(memory_space=pltpu.SMEM)
        attn_send, k_out, v_out = pl.pallas_call(
            functools.partial(attention_kernel, heads, qkv_dev),
            out_shape=(
                jax.ShapeDtypeStruct((NDEV, batch_dev, LANES), BF16),
                jax.ShapeDtypeStruct(k_loc.shape, BF16),
                jax.ShapeDtypeStruct(v_loc.shape, BF16),
            ),
            in_specs=[smem, vmem, vmem, vmem, anym, anym],
            out_specs=(vmem, anym, anym),
            scratch_shapes=[
                pltpu.VMEM(k_loc.shape, BF16),
                pltpu.VMEM(v_loc.shape, BF16),
                pltpu.VMEM((batch_dev * steps * heads, head_dim), F32),
                pltpu.VMEM((steps * batch_dev, head_dim), F32),
                pltpu.VMEM((steps * batch_dev, head_dim), F32),
                pltpu.VMEM((NDEV * batch_dev, LANES), F32),
                dma((2, batch_dev)),
                dma((2, batch_dev)),
            ],
            compiler_params=pltpu.CompilerParams(vmem_limit_bytes=KERNEL_VMEM),
            cost_estimate=pl.CostEstimate(flops=1_000_000_000, bytes_accessed=34_000_000, transcendentals=0),
            name="attention",
        )(own_lens, qkv_parts, cosine, sine, k_loc, v_loc)

        next_rows = next_ids.reshape(pair_dims).transpose(0, 2, 1, 3).reshape(PIECES, piece_rows)
        log_probs = pl.pallas_call(
            functools.partial(back_kernel, vocab_dev, width, attn_dev, ff_dev, width ** -0.5),
            out_shape=jax.ShapeDtypeStruct((2 * PIECES, LANES), F32),
            in_specs=[vmem, vmem, vmem, vmem, vmem, anym, anym],
            out_specs=vmem,
            scratch_shapes=[
                pltpu.VMEM((vocab_dev, width), BF16),
                pltpu.VMEM((2 * attn_dev, width), BF16),
                pltpu.VMEM((ff_dev, width), BF16),
                pltpu.VMEM((NDEV, batch_dev, LANES), BF16),
                pltpu.VMEM((PIECES, 8, piece_rows), F32),
                pltpu.VMEM((PIECES, 8, 8, LANES), F32),
                pltpu.VMEM((PIECES, NZ, 8, LANES), F32),
                dma((4,)),
                dma((NDEV,)),
                dma((NDEV,)),
                dma((PIECES, 12)),
                dma((PIECES, 12)),
            ] + exchange,
            compiler_params=pltpu.CompilerParams(collective_id=1, has_side_effects=True, vmem_limit_bytes=KERNEL_VMEM),
            cost_estimate=pl.CostEstimate(flops=40_000_000_000, bytes_accessed=8_000_000, transcendentals=0),
            name="back",
        )(attn_send, mlp, x_own, final_gain, next_rows, w_out_loc, embed_loc)
        log_probs = log_probs.reshape(steps, HALVES, NDEV, ROWS).transpose(0, 2, 1, 3).reshape(steps, batch)
        return log_probs, k_out, v_out

    cache_spec = P('tp', None, None)
    return jax.shard_map(device_fn, mesh=mesh, in_specs=(P(), P(), P(), P('tp', None), P(), P(None, 'tp'), P('tp', None), P(), cache_spec, cache_spec), out_specs=(P(), cache_spec, cache_spec), check_vma=False)
```
